256 devices in a mesh: slab: 64 (over z, x, core), sub: 4 (over y).
Axes of the slice: x: 4, y: 4, z: 8, core: 2. Of those that a mesh axis runs over, the one named last changes fastest.
Arguments:
- values: float32 [6144, 2, 128, 256], P(('slab', 'sub')), may hold values from -0.25 to 0.25
- block_ids: int32 [6144, 2], P(('slab', 'sub')), may hold values from 0 to 3071, as said below
- tile_counts: int32 [64, 4], P('slab', 'sub'), may hold values from 8 to 24, as said below
- right_side: float32 [6144, 128], P(('slab', 'sub')), may hold values from -18 to 18
Outputs:
- solution: float32 [3072, 256], P(('slab', 'sub'))
- residual: float32 [6144, 128], P(('slab', 'sub'))
The draws below stay inside these ranges and needn't reach their ends.
Inputs may be any that keep to these rules, and one draw needn't show every extreme that they name: `block_ids`: every block id names a node block held by a device of the row tile's own slab or of a slab one index of slab away; the first coupled block of each tile lies in its own slab. Block b is held by device b div 12. `tile_counts`: some device has all 24 slots live in every draw.
All inputs are finite; a program needn't handle non-finite values.
Results may differ from the reference program's by a relative error of at most 0.0003.
Values sent between devices are 32-bit elements; how exact they have to be, the bound alone decides.
A program may use at most 64 MiB of HBM per device.

```python
import jax
import jax.numpy as jnp
from jax import lax

BLOCK = 256
TILE_ROWS = 128
COUPLED = 2
ITERS = 4
TILES_DEV = 24
NB_DEV = 12
TILES = 6144
NBLOCKS = 3072
N_SLAB = 64
N_SUB = 4


def draw_block_ids(key, part):
    tile_slab = jnp.arange(TILES, dtype=jnp.int32) // TILES_DEV // N_SUB
    offset = jax.random.randint(jax.random.fold_in(key, 11), (TILES, COUPLED), -1, 2)
    first_slot = jnp.arange(COUPLED, dtype=jnp.int32)[None, :] == 0
    offset = jnp.where(first_slot, 0, offset)
    other_slab = jnp.clip(tile_slab[:, None] + offset, 0, N_SLAB - 1)
    owner_sub = jax.random.randint(jax.random.fold_in(key, 12), (TILES, COUPLED), 0, N_SUB)
    slot_index = jax.random.randint(jax.random.fold_in(key, 13), (TILES, COUPLED), 0, NB_DEV)
    return ((other_slab * N_SUB + owner_sub) * NB_DEV + slot_index).astype(jnp.int32)


def draw_tile_counts(key, part):
    lowest = TILES_DEV // 3
    counts = jax.random.randint(jax.random.fold_in(key, 21), (N_SLAB * N_SUB,), lowest, TILES_DEV + 1)
    fuller = jax.random.randint(jax.random.fold_in(key, 22), (), 0, N_SLAB * N_SUB)
    counts = jnp.where(jnp.arange(N_SLAB * N_SUB, dtype=jnp.int32) == fuller, TILES_DEV, counts)
    return counts.reshape(N_SLAB, N_SUB).astype(jnp.int32)


def draw_right_side(key, part):
    position = jnp.arange(TILES, dtype=jnp.float32) / max(TILES - 1, 1)
    base = jnp.clip(jax.random.normal(jax.random.fold_in(key, 32), (TILES, TILE_ROWS), jnp.float32), -6.0, 6.0)
    rising = 1.0 + 2.0 * position
    return (base * rising[:, None]).astype(jnp.float32)


def steps_of(stream_key, extent, shards, smallest, top_value):
    level = 1.0
    for dim, parts in shards:
        heights = jax.random.uniform(jax.random.fold_in(jax.random.fold_in(stream_key, 6), dim), (parts,), jnp.float32, smallest / len(shards), top_value / len(shards))
        level = level * jnp.repeat(jnp.exp(heights), extent[dim] // parts).reshape((-1,) + (1,) * (len(extent) - 1 - dim))
    return level


def bell_draw(key, extent, width, reach, split=(), held_as=jnp.bfloat16):
    entries = jax.random.normal(key, extent, jnp.float32) * width
    if len(split) > 0:
        entries = steps_of(key, extent, split, -0.22, 0.18) * entries
    return jnp.clip(entries, min=-reach, max=reach).astype(held_as)


def setup_inputs(seed: int = 0) -> dict:
    key_list = jax.random.split(jax.random.key(seed), 5)
    return {
        "values": bell_draw(key_list[0], (TILES, COUPLED, TILE_ROWS, BLOCK), (COUPLED * BLOCK) ** -0.5, 0.25, ((0, 256),), jnp.float32),
        "block_ids": draw_block_ids(jax.random.fold_in(key_list[4], 71), 0),
        "tile_counts": draw_tile_counts(jax.random.fold_in(key_list[4], 71), 0),
        "right_side": draw_right_side(jax.random.fold_in(key_list[4], 71), 0),
    }


precise = lax.Precision.HIGHEST


def live_mask(tile_counts):
    position = jnp.arange(TILES, dtype=jnp.int32)
    owner_dev = (position // TILES_DEV).astype(jnp.int32)
    limit = tile_counts.reshape(-1)[owner_dev]
    return ((position % TILES_DEV) < limit).astype(jnp.float32)


def forward(values, block_ids, live_tiles, field):
    picked = field[block_ids]
    image = jnp.einsum("tkij,tkj->ti", values, picked, precision=precise)
    return image * live_tiles[:, None]


def backward(values, block_ids, rows):
    terms = jnp.einsum("tkij,ti->tkj", values, rows, precision=precise)
    return jax.ops.segment_sum(terms.reshape(-1, BLOCK), block_ids.reshape(-1), num_segments=NBLOCKS)


def reference(values, block_ids, tile_counts, right_side):
    live_tiles = live_mask(tile_counts)
    squares = jnp.einsum("tkij,tkij->tkj", values, values, precision=precise) * live_tiles[:, None, None]
    col_squares = jax.ops.segment_sum(squares.reshape(-1, BLOCK), block_ids.reshape(-1), num_segments=NBLOCKS)
    jacobi = 1.0 / (1.0 + col_squares)
    solution = jnp.zeros((NBLOCKS, BLOCK), jnp.float32)
    residual = right_side * live_tiles[:, None]
    normal_res = backward(values, block_ids, residual)
    scaled = jacobi * normal_res
    direction = scaled
    rho_now = jnp.sum(normal_res * scaled)
    for iteration in range(ITERS):
        image = forward(values, block_ids, live_tiles, direction)
        step_size = rho_now / jnp.sum(image * image)
        solution = solution + step_size * direction
        residual = residual - step_size * image
        normal_res = backward(values, block_ids, residual)
        scaled = jacobi * normal_res
        rho_next = jnp.sum(normal_res * scaled)
        direction = scaled + (rho_next / rho_now) * direction
        rho_now = rho_next
    return (solution, residual)
```

```python
import functools

import jax
import jax.numpy as jnp
from jax import lax
from jax.experimental import pallas as pl
from jax.experimental.pallas import tpu as pltpu
from jax.sharding import PartitionSpec as P

MESH = pl.DeviceIdType.MESH
NODES = 12
XGROUP = 8
CHUNKS = 4
F32 = jnp.float32
BF16 = jnp.bfloat16


def total(value):
    return jnp.sum(jnp.sum(value, axis=1, keepdims=True), axis=0, keepdims=True)


def packed(parts):
    lanes = lax.broadcasted_iota(jnp.int32, (1, 128), 1)
    row = jnp.zeros((1, 128), F32)
    for place, part in enumerate(parts):
        row = jnp.where(lanes == place, part, row)
    return row


def unpacked(row, count):
    lanes = lax.broadcasted_iota(jnp.int32, (1, 128), 1)
    return [
        jnp.sum(jnp.where(lanes == place, row, 0.0), axis=1, keepdims=True) for place in range(count)
    ]


def kernel(
    slabs,
    subs,
    xgroup,
    ids_ref,
    count_ref,
    values_hbm,
    side_ref,
    solution_ref,
    residual_ref,
    values,
    ids_buf,
    first_terms,
    terms,
    first_sums,
    sums,
    first_near,
    first_far,
    near,
    far,
    window,
    rows,
    xred,
    zred,
    yred,
    load_sem,
    ids_send,
    ids_recv,
    term_send,
    term_recv,
    sum_send,
    sum_recv,
    x_send,
    x_recv,
    z_send,
    z_recv,
    y_send,
    y_recv,
):
    tiles = values.shape[0]
    width = values.shape[3]
    own = 2 * tiles
    nodes = subs * NODES
    slab = lax.axis_index("slab")
    sub = lax.axis_index("sub")
    zgroup = slabs // xgroup
    x_place = lax.rem(slab, xgroup)
    z_place = slab // xgroup

    def sub_peer(step):
        return (slab, lax.rem(sub + step, subs))

    def slab_peer(step):
        return (lax.rem(slab + step + slabs, slabs), sub)

    def x_peer(step):
        return (z_place * xgroup + lax.rem(x_place + step, xgroup), sub)

    def z_peer(step):
        return (lax.rem(z_place + step, zgroup) * xgroup + x_place, sub)

    chunk = tiles // CHUNKS
    loads = [
        pltpu.make_async_copy(
            values_hbm.at[pl.ds(part * chunk, chunk)],
            values.at[pl.ds(part * chunk, chunk)],
            load_sem.at[part],
        )
        for part in range(CHUNKS)
    ]
    for load in loads:
        load.start()

    barrier = pltpu.get_barrier_semaphore()
    partners = (
        [sub_peer(step) for step in range(1, subs)]
        + [slab_peer(step) for step in (-2, -1, 1, 2)]
        + [x_peer(step) for step in range(1, xgroup)]
        + [z_peer(step) for step in range(1, zgroup)]
    )
    for partner in partners:
        pl.semaphore_signal(barrier, inc=1, device_id=partner, device_id_type=MESH)

    base = (slab - 1) * nodes
    count = count_ref[0, 0]
    lanes = lax.broadcasted_iota(jnp.int32, (1, 256), 1)
    ids_row = jnp.zeros((1, 256), jnp.int32)
    for tile in range(tiles):
        for slot in range(2):
            mark = ids_ref[tile, slot] - base + 1
            ids_row = jnp.where(lanes == sub * own + 2 * tile + slot, mark, ids_row)
    ids_buf[sub] = ids_row

    live_rows = lax.broadcasted_iota(jnp.int32, (tiles, 128), 0) < count
    residual = jnp.where(live_rows, side_ref[...], 0.0)
    rows[...] = residual
    eye = lax.broadcasted_iota(jnp.int32, (128, 128), 0) == lax.broadcasted_iota(
        jnp.int32, (128, 128), 1
    )

    def copy(source, target, send, recv, peer):
        return pltpu.make_async_remote_copy(
            src_ref=source,
            dst_ref=target,
            send_sem=send,
            recv_sem=recv,
            device_id=peer,
            device_id_type=MESH,
        )

    def live_of(tile):
        return jnp.where(tile < count, 1.0, 0.0).astype(F32)

    def first_tile(tile):
        live = live_of(tile)
        column = jnp.sum(
            jnp.where(eye, rows[pl.ds(tile, 1), :], 0.0), axis=1, keepdims=True
        )
        for slot in range(2):
            block = values[tile, slot]
            at = sub * own + 2 * tile + slot
            first_terms[0, pl.ds(at, 1), :] = jnp.sum(block * column, axis=0, keepdims=True)
            first_terms[1, pl.ds(at, 1), :] = jnp.sum(block * block, axis=0, keepdims=True) * live

    def picked(tile, slot):
        at = jnp.minimum(jnp.maximum(ids_ref[tile, slot] - base, 0), 3 * nodes - 1)
        return window[pl.ds(at, 1), :]

    def image_of(tile):
        live = live_of(tile)
        low = picked(tile, 0) * live
        high = picked(tile, 1) * live
        product = values[tile, 0] * low + values[tile, 1] * high
        folded = sum(product[:, 128 * i : 128 * (i + 1)] for i in range(width // 128))
        column = jnp.sum(folded, axis=1, keepdims=True)
        rows[pl.ds(tile, 1), :] = jnp.sum(jnp.where(eye, column, 0.0), axis=0, keepdims=True)
        return column

    def full_tile(step, tile):
        column = image_of(tile)
        for slot in range(2):
            at = sub * own + 2 * tile + slot
            terms[step, pl.ds(at, 1), :] = jnp.sum(
                values[tile, slot] * column, axis=0, keepdims=True
            )

    def wait_barrier():
        pl.semaphore_wait(barrier, len(partners))

    def own_rows(ref, step):
        return ref.at[step, pl.ds(sub * own, own)]

    for part in range(CHUNKS):
        loads[part].wait()

        @pl.loop(part * chunk, (part + 1) * chunk, unroll=2)
        def _(tile):
            first_tile(tile)

    wait_barrier()
    sent = []
    for step in range(1, subs):
        place = lax.rem(sub, subs)
        peer = sub_peer(step)
        item = copy(ids_buf.at[sub], ids_buf.at[sub], ids_send.at[step], ids_recv.at[step], peer)
        item.start()
        sent.append(item)
        for part in range(2):
            item = copy(
                own_rows(first_terms, part),
                own_rows(first_terms, part),
                term_send.at[3 + part, step],
                term_recv.at[3 + part, step],
                peer,
            )
            item.start()
            sent.append(item)
    for item in sent:
        item.wait_recv()

    all_ids = sum(ids_buf[i] for i in range(subs))[:, : subs * own]
    row_ids = lax.broadcasted_iota(jnp.int32, (3 * nodes, subs * own), 0) + 1
    selector = jnp.where(row_ids == all_ids, 1.0, 0.0).astype(BF16)

    def summed(value):
        high = value.astype(BF16)
        rest = value - high.astype(F32)
        middle = rest.astype(BF16)
        low = (rest - middle.astype(F32)).astype(BF16)
        return sum(
            jnp.dot(selector, piece, preferred_element_type=F32) for piece in (high, middle, low)
        )

    def exchange(sum_ref, near_ref, far_ref, index):
        moves = (
            (1, pl.ds(nodes, 2 * nodes), near_ref.at[0]),
            (-1, pl.ds(0, 2 * nodes), near_ref.at[1]),
            (2, pl.ds(2 * nodes, nodes), far_ref.at[0]),
            (-2, pl.ds(0, nodes), far_ref.at[1]),
        )
        items = []
        for place, (step, part, target) in enumerate(moves):
            item = copy(
                sum_ref.at[part],
                target,
                sum_send.at[index, place],
                sum_recv.at[index, place],
                slab_peer(step),
            )
            item.start()
            items.append(item)
        return items

    def combined(mine, near_ref, far_ref):
        below, above = near_ref[0], near_ref[1]
        return jnp.concatenate(
            [
                (far_ref[0] + below[:nodes]) + mine[:nodes],
                (below[nodes:] + mine[nodes : 2 * nodes]) + above[:nodes],
                (mine[2 * nodes :] + above[nodes:]) + far_ref[1],
            ],
            axis=0,
        )

    mine = []
    for part in range(2):
        mine.append(summed(first_terms[part]))
        first_sums[part] = mine[part]
        sent += exchange(first_sums.at[part], first_near.at[part], first_far.at[part], 3 + part)
    for item in sent[-8:]:
        item.wait_recv()
    normal = combined(mine[0], first_near.at[0], first_far.at[0])
    squares = combined(mine[1], first_near.at[1], first_far.at[1])
    jacobi = 1.0 / (1.0 + squares)

    def middle_of(value):
        return value[nodes : 2 * nodes]

    def start_x(index, row):
        xred[index, x_place] = row
        items = []
        for step in range(1, xgroup):
            item = copy(
                xred.at[index, x_place],
                xred.at[index, x_place],
                x_send.at[index, step],
                x_recv.at[index, step],
                x_peer(step),
            )
            item.start()
            items.append(item)
        return items

    def turn_to_z(index, items):
        for item in items:
            item.wait_recv()
        row = jnp.sum(xred[index], axis=0)
        zred[index, z_place] = row
        later = []
        for step in range(1, zgroup):
            item = copy(
                zred.at[index, z_place],
                zred.at[index, z_place],
                z_send.at[index, step],
                z_recv.at[index, step],
                z_peer(step),
            )
            item.start()
            later.append(item)
        return later

    def finish_z(index, items):
        for item in items:
            item.wait_recv()
        return jnp.sum(zred[index], axis=0)

    def applied(step, pending):
        @pl.loop(0, tiles, unroll=4)
        def _(tile):
            full_tile(step, tile)

        items = []
        for peer_step in range(1, subs):
            item = copy(
                own_rows(terms, step),
                own_rows(terms, step),
                term_send.at[step, peer_step],
                term_recv.at[step, peer_step],
                sub_peer(peer_step),
            )
            item.start()
            items.append(item)
        later = []
        if pending is not None:
            later = turn_to_z(*pending)
        for item in items:
            item.wait_recv()
        here = summed(terms[step])
        sums[step] = here
        moved = exchange(sums.at[step], near.at[step], far.at[step], step)
        for item in moved:
            item.wait_recv()
        sent.extend(items + later + moved)
        return combined(here, near.at[step], far.at[step]), later

    u_all = jacobi * normal
    window[...] = u_all
    w_all, _ = applied(0, None)
    a_row = rows[...]
    r, u = middle_of(normal), middle_of(u_all)
    w = middle_of(w_all)
    items = start_x(0, packed([total(r * u), total(w * u)]))
    sent += items
    m_all = jacobi * w_all
    window[...] = m_all

    n_all, later = applied(1, (0, items))
    g_row = rows[...]
    rho_0, norm_0 = unpacked(finish_z(0, later), 2)
    alpha = rho_0 / norm_0
    z_all = n_all
    q, s, p = middle_of(m_all), w, u
    ap_row, aq_row = a_row, g_row
    w_all = w_all - alpha * z_all
    m_all = jacobi * w_all
    window[...] = m_all
    x = alpha * p
    r = r - alpha * s
    u = u - alpha * q
    residual = residual - alpha * ap_row
    a_row = a_row - alpha * aq_row
    w = middle_of(w_all)
    items = start_x(1, packed([total(r * u), total(w * u), total(w * p)]))
    sent += items

    n_all, later = applied(2, (1, items))
    g_row = rows[...]
    rho_1, uu, cross = unpacked(finish_z(1, later), 3)
    beta = rho_1 / rho_0
    norm_1 = uu + 2.0 * beta * cross + beta * beta * norm_0
    alpha = rho_1 / norm_1
    z_all = n_all + beta * z_all
    m = middle_of(m_all)
    w_all = w_all - alpha * z_all
    q = m + beta * q
    s = w + beta * s
    p = u + beta * p
    m_all = jacobi * w_all
    window[...] = m_all
    x = x + alpha * p
    r = r - alpha * s
    u = u - alpha * q
    ap_row = a_row + beta * ap_row
    aq_row = g_row + beta * aq_row
    residual = residual - alpha * ap_row
    a_row = a_row - alpha * aq_row
    w, m = middle_of(w_all), middle_of(m_all)

    @pl.loop(0, tiles, unroll=4)
    def _(tile):
        image_of(tile)

    g_row = rows[...]
    fields = [a_row, g_row, aq_row, ap_row]
    pairs = [(i, j) for i in range(4) for j in range(i, 4)]
    row_part = packed([total(fields[i] * fields[j]) for i, j in pairs])
    node_dots = [
        total(r * u),
        total(w * u),
        total(w * p),
        total(s * u),
        total(w * m),
        total(s * m),
        total(s * q),
    ]
    place = lax.broadcasted_iota(jnp.int32, (1, 128), 1)
    node_part = jnp.zeros((1, 128), F32)
    for index, part in enumerate(node_dots):
        node_part = jnp.where(place == len(pairs) + index, part, node_part)
    yred[sub] = row_part
    items = []
    for step in range(1, subs):
        item = copy(
            yred.at[sub], yred.at[sub], y_send.at[step], y_recv.at[step], sub_peer(step)
        )
        item.start()
        items.append(item)
    sent += items
    for item in items:
        item.wait_recv()
    items = start_x(2, jnp.sum(yred[...], axis=0) + node_part)
    sent += items
    later = turn_to_z(2, items)
    sent += later
    found = unpacked(finish_z(2, later), len(pairs) + len(node_dots))
    gram = dict(zip(pairs, found[: len(pairs)]))
    rho_2, uu, cross, s_u, w_m, s_m, s_q = found[len(pairs) :]
    beta = rho_2 / rho_1
    norm_2 = uu + 2.0 * beta * cross + beta * beta * norm_1
    alpha = rho_2 / norm_2
    rho_3 = (
        rho_2
        - 2.0 * alpha * (uu + beta * s_u)
        + alpha * alpha * (w_m + 2.0 * beta * s_m + beta * beta * s_q)
    )
    beta_3 = rho_3 / rho_2
    weights = [1.0 + beta_3, -alpha, -alpha * beta, beta_3 * beta]
    norm_3 = 0.0
    for i, j in pairs:
        norm_3 = norm_3 + (1.0 if i == j else 2.0) * weights[i] * weights[j] * gram[i, j]
    alpha_3 = rho_3 / norm_3
    p = u + beta * p
    x = x + alpha * p
    u = u - alpha * (m + beta * q)
    p = u + beta_3 * p
    x = x + alpha_3 * p
    ap_row = a_row + beta * ap_row
    last_row = sum(weights[i] * fields[i] for i in range(4))
    residual = residual - alpha * ap_row - alpha_3 * last_row
    residual_ref[...] = residual
    mine = x[:NODES]
    for index in range(1, subs):
        mine = jnp.where(sub == index, x[index * NODES : (index + 1) * NODES], mine)
    solution_ref[...] = mine
    for item in sent:
        item.wait_send()


def per_device(slabs, subs, values, block_ids, tile_counts, right_side):
    tiles, coupled, height, width = values.shape
    own = 2 * tiles
    nodes = subs * NODES
    xgroup = min(XGROUP, slabs // 2)
    zgroup = slabs // xgroup
    vmem = pltpu.VMEM
    dma = pltpu.SemaphoreType.DMA
    return pl.pallas_call(
        functools.partial(kernel, slabs, subs, xgroup),
        out_shape=(
            jax.ShapeDtypeStruct((NODES, width), F32),
            jax.ShapeDtypeStruct((tiles, height), F32),
        ),
        in_specs=[
            pl.BlockSpec(memory_space=pltpu.SMEM),
            pl.BlockSpec(memory_space=pltpu.SMEM),
            pl.BlockSpec(memory_space=pl.ANY),
            pl.BlockSpec(memory_space=pltpu.VMEM),
        ],
        out_specs=(
            pl.BlockSpec(memory_space=pltpu.VMEM),
            pl.BlockSpec(memory_space=pltpu.VMEM),
        ),
        scratch_shapes=[
            vmem(values.shape, F32),
            vmem((subs, 1, 256), jnp.int32),
            vmem((2, subs * own, width), F32),
            vmem((3, subs * own, width), F32),
            vmem((2, 3 * nodes, width), F32),
            vmem((3, 3 * nodes, width), F32),
            vmem((2, 2, 2 * nodes, width), F32),
            vmem((2, 2, nodes, width), F32),
            vmem((3, 2, 2 * nodes, width), F32),
            vmem((3, 2, nodes, width), F32),
            vmem((3 * nodes, width), F32),
            vmem((tiles, height), F32),
            vmem((3, xgroup, 1, 128), F32),
            vmem((3, zgroup, 1, 128), F32),
            vmem((subs, 1, 128), F32),
            dma((CHUNKS,)),
            dma((subs,)),
            dma((subs,)),
            dma((5, subs)),
            dma((5, subs)),
            dma((5, 4)),
            dma((5, 4)),
            dma((3, xgroup)),
            dma((3, xgroup)),
            dma((3, zgroup)),
            dma((3, zgroup)),
            dma((subs,)),
            dma((subs,)),
        ],
        compiler_params=pltpu.CompilerParams(
            collective_id=0, has_side_effects=True, vmem_limit_bytes=48 * 1024 * 1024
        ),
        name="cgls",
    )(block_ids, tile_counts, values, right_side)


def solution(mesh):
    both = ("slab", "sub")
    return jax.shard_map(
        functools.partial(per_device, mesh.shape["slab"], mesh.shape["sub"]),
        mesh=mesh,
        in_specs=(P(both, None, None, None), P(both, None), P("slab", "sub"), P(both, None)),
        out_specs=(P(both, None), P(both, None)),
        check_vma=False,
    )
```

```python
import functools

import jax
import jax.numpy as jnp
from jax import lax
from jax.experimental import pallas as pl
from jax.experimental.pallas import tpu as pltpu
from jax.sharding import PartitionSpec as P

MESH = pl.DeviceIdType.MESH
NODES = 12
CORES = 2
ALONG_X = 4
GROUPS = 3
F32 = jnp.float32
BF16 = jnp.bfloat16


def total(value):
    return jnp.sum(jnp.sum(value, axis=1, keepdims=True), axis=0, keepdims=True)


def packed(parts):
    lanes = lax.broadcasted_iota(jnp.int32, (1, 128), 1)
    row = jnp.zeros((1, 128), F32)
    for place, part in enumerate(parts):
        row = jnp.where(lanes == place, part, row)
    return row


def unpacked(row, count):
    lanes = lax.broadcasted_iota(jnp.int32, (1, 128), 1)
    return [
        jnp.sum(jnp.where(lanes == place, row, 0.0), axis=1, keepdims=True) for place in range(count)
    ]


def kernel(
    slabs,
    subs,
    along_x,
    ids_hbm,
    count_ref,
    values_hbm,
    side_hbm,
    solution_ref,
    residual_ref,
    values,
    side,
    ids_ref,
    columns,
    ids_buf,
    first_terms,
    terms,
    first_sums,
    sums,
    first_near,
    first_far,
    near,
    far,
    window,
    rows,
    plane,
    depth,
    load_sem,
    side_sem,
    index_sem,
    ids_send,
    ids_recv,
    term_send,
    term_recv,
    sum_send,
    sum_recv,
    plane_send,
    plane_recv,
    depth_send,
    depth_recv,
):
    tiles = values.shape[0]
    own = 2 * tiles
    nodes = subs * NODES
    slab = lax.axis_index("slab")
    sub = lax.axis_index("sub")
    along_z = slabs // (along_x * CORES)
    core = lax.rem(slab, CORES)
    x_at = lax.rem(slab // CORES, along_x)
    z_at = slab // (CORES * along_x)
    plane_count = along_x * subs
    depth_count = along_z * CORES
    plane_at = x_at * subs + sub
    depth_at = z_at * CORES + core

    def sub_peer(step):
        return (slab, lax.rem(sub + step, subs))

    def slab_peer(step):
        return (lax.rem(slab + step + slabs, slabs), sub)

    def plane_peer(step):
        at = lax.rem(plane_at + step, plane_count)
        return ((z_at * along_x + at // subs) * CORES + core, lax.rem(at, subs))

    def depth_peer(step):
        at = lax.rem(depth_at + step, depth_count)
        return ((at // CORES * along_x + x_at) * CORES + lax.rem(at, CORES), sub)

    def half_of(half):
        return pl.ds(128 * half, 128)

    group = tiles // GROUPS
    side_load = pltpu.make_async_copy(side_hbm, side, side_sem)
    side_load.start()
    ids_load = pltpu.make_async_copy(ids_hbm, ids_ref, index_sem)
    ids_load.start()
    loads = []
    for half in range(2):
        for part in range(GROUPS):
            at = (pl.ds(part * group, group), slice(None), slice(None), half_of(half))
            loads.append(
                pltpu.make_async_copy(
                    values_hbm.at[at], values.at[at], load_sem.at[half * GROUPS + part]
                )
            )
    for load in loads:
        load.start()

    barrier = pltpu.get_barrier_semaphore()
    partners = (
        [slab_peer(step) for step in (-2, -1, 1, 2)]
        + [plane_peer(step) for step in range(1, plane_count)]
        + [depth_peer(step) for step in range(1, depth_count)]
    )
    for partner in partners:
        pl.semaphore_signal(barrier, inc=1, device_id=partner, device_id_type=MESH)

    base = (slab - 1) * nodes
    count = count_ref[0, 0]
    ids_load.wait()
    lanes = lax.broadcasted_iota(jnp.int32, (1, 256), 1)
    ids_row = jnp.zeros((1, 256), jnp.int32)
    for tile in range(tiles):
        for slot in range(2):
            mark = ids_ref[slot, tile] - base + 1
            ids_row = jnp.where(lanes == sub * own + 2 * tile + slot, mark, ids_row)
    ids_buf[sub] = ids_row

    live_rows = lax.broadcasted_iota(jnp.int32, (tiles, 128), 0) < count
    side_load.wait()
    residual = jnp.where(live_rows, side[...], 0.0)
    rows[...] = residual
    eye = lax.broadcasted_iota(jnp.int32, (128, 128), 0) == lax.broadcasted_iota(
        jnp.int32, (128, 128), 1
    )
    sent = []

    def copy(source, target, send, recv, peer):
        item = pltpu.make_async_remote_copy(
            src_ref=source,
            dst_ref=target,
            send_sem=send,
            recv_sem=recv,
            device_id=peer,
            device_id_type=MESH,
        )
        item.start()
        sent.append(item)
        return item

    def live_of(tile):
        return jnp.where(tile < count, 1.0, 0.0).astype(F32)

    def place_of(tile, slot):
        return pl.ds(sub * own + 2 * tile + slot, 1)

    def first_tile(tile, half):
        live = live_of(tile)
        if half == 0:
            column = jnp.sum(
                jnp.where(eye, rows[pl.ds(tile, 1), :], 0.0), axis=1, keepdims=True
            )
            column = jnp.broadcast_to(column, (128, 128))
            columns[tile] = column
        else:
            column = columns[tile]
        for slot in range(2):
            block = values[tile, slot, :, 128 * half : 128 * (half + 1)]
            at = place_of(tile, slot)
            first_terms[half, 0, at, :] = jnp.sum(block * column, axis=0, keepdims=True)
            first_terms[half, 1, at, :] = jnp.sum(block * block, axis=0, keepdims=True) * live

    def image_of(tile):
        live = live_of(tile)
        product = None
        for slot in range(2):
            at = jnp.minimum(jnp.maximum(ids_ref[slot, tile] - base, 0), 3 * nodes - 1)
            for half in range(2):
                row = window[half, pl.ds(at, 1), :] * live
                part = values[tile, slot, :, 128 * half : 128 * (half + 1)] * row
                product = part if product is None else product + part
        column = jnp.sum(product, axis=1, keepdims=True)
        rows[pl.ds(tile, 1), :] = jnp.sum(jnp.where(eye, column, 0.0), axis=0, keepdims=True)
        return column

    def back_tile(phase, tile, half):
        if half == 0:
            column = jnp.broadcast_to(image_of(tile), (128, 128))
            columns[tile] = column
        else:
            column = columns[tile]
        for slot in range(2):
            block = values[tile, slot, :, 128 * half : 128 * (half + 1)]
            terms[phase, half, 0, place_of(tile, slot), :] = jnp.sum(
                block * column, axis=0, keepdims=True
            )

    def spread(terms_ref, phase, half):
        part = terms_ref.at[half, :, pl.ds(sub * own, own)]
        return [
            copy(
                part,
                part,
                term_send.at[phase, half, step],
                term_recv.at[phase, half, step],
                sub_peer(step),
            )
            for step in range(1, subs)
        ]

    def arrived(items):
        for item in items:
            item.wait_recv()

    def summed(value):
        high = value.astype(BF16)
        rest = value - high.astype(F32)
        middle = rest.astype(BF16)
        low = (rest - middle.astype(F32)).astype(BF16)
        return sum(
            jnp.dot(selector, piece, preferred_element_type=F32) for piece in (high, middle, low)
        )

    def exchange(terms_ref, sums_ref, near_ref, far_ref, phase, half):
        mine = []
        for index in range(terms_ref.shape[1]):
            mine.append(summed(terms_ref[half, index]))
            sums_ref[half, index] = mine[index]
        moves = (
            (1, pl.ds(nodes, 2 * nodes), near_ref.at[half, 0]),
            (-1, pl.ds(0, 2 * nodes), near_ref.at[half, 1]),
            (2, pl.ds(2 * nodes, nodes), far_ref.at[half, 0]),
            (-2, pl.ds(0, nodes), far_ref.at[half, 1]),
        )
        items = [
            copy(
                sums_ref.at[half, :, part],
                target,
                sum_send.at[phase, half, place],
                sum_recv.at[phase, half, place],
                slab_peer(step),
            )
            for place, (step, part, target) in enumerate(moves)
        ]
        return mine, items

    def combined(mine, near_ref, far_ref, half):
        found = []
        for index, value in enumerate(mine):
            below, above = near_ref[half, 0, index], near_ref[half, 1, index]
            found.append(
                jnp.concatenate(
                    [
                        (far_ref[half, 0, index] + below[:nodes]) + value[:nodes],
                        (below[nodes:] + value[nodes : 2 * nodes]) + above[:nodes],
                        (value[2 * nodes :] + above[nodes:]) + far_ref[half, 1, index],
                    ],
                    axis=0,
                )
            )
        return found

    def start_plane(index, row):
        plane[index, plane_at] = row
        at = plane.at[index, plane_at]
        return [
            copy(at, at, plane_send.at[index, step], plane_recv.at[index, step], plane_peer(step))
            for step in range(1, plane_count)
        ]

    def start_depth(index, items):
        arrived(items)
        depth[index, depth_at] = jnp.sum(plane[index], axis=0)
        at = depth.at[index, depth_at]
        return [
            copy(at, at, depth_send.at[index, step], depth_recv.at[index, step], depth_peer(step))
            for step in range(1, depth_count)
        ]

    def finish_depth(index, items, number):
        arrived(items)
        return unpacked(jnp.sum(depth[index], axis=0), number)

    def middle_of(halves):
        return [half[nodes : 2 * nodes] for half in halves]

    def dot(one, other):
        return total(one[0] * other[0] + one[1] * other[1]) * (1.0 / subs)

    items = []
    for half in range(2):
        for part in range(GROUPS):
            loads[half * GROUPS + part].wait()

            @pl.loop(part * group, (part + 1) * group, unroll=2)
            def _(tile):
                first_tile(tile, half)

        if half == 0:
            pl.semaphore_wait(barrier, len(partners))
            place = ids_buf.at[sub]
            ids_items = [
                copy(place, place, ids_send.at[step], ids_recv.at[step], sub_peer(step))
                for step in range(1, subs)
            ]
        items.append(spread(first_terms, 0, half))
    arrived(ids_items)
    all_ids = sum(ids_buf[i] for i in range(subs))[:, : subs * own]
    row_ids = lax.broadcasted_iota(jnp.int32, (3 * nodes, subs * own), 0) + 1
    selector = jnp.where(row_ids == all_ids, 1.0, 0.0).astype(BF16)
    moved = []
    for half in range(2):
        arrived(items[half])
        moved.append(exchange(first_terms, first_sums, first_near, first_far, 0, half))
    normal, jacobi, u_all = [], [], []
    for half in range(2):
        mine, items = moved[half]
        arrived(items)
        found, squares = combined(mine, first_near, first_far, half)
        normal.append(found)
        jacobi.append(1.0 / (1.0 + squares))
        u_all.append(jacobi[half] * found)
        window[half] = u_all[half]

    def applied(phase, dots):
        items = []
        for half in range(2):

            @pl.loop(0, tiles, unroll=4)
            def _(tile):
                back_tile(phase, tile, half)

            items.append(spread(terms.at[phase], 1 + phase, half))
        later = dots() if dots is not None else None
        moved = []
        for half in range(2):
            arrived(items[half])
            moved.append(
                exchange(
                    terms.at[phase],
                    sums.at[phase],
                    near.at[phase],
                    far.at[phase],
                    1 + phase,
                    half,
                )
            )
        return moved, later

    def result(phase, moved, half):
        mine, items = moved[half]
        arrived(items)
        return combined(mine, near.at[phase], far.at[phase], half)[0]

    r, u = middle_of(normal), middle_of(u_all)

    def dots_0():
        a_row = rows[...]
        return start_plane(0, packed([dot(r, u), total(a_row * a_row)]))

    moved, reducing = applied(0, dots_0)
    a_row = rows[...]
    w_all, m_all = [], []
    for half in range(2):
        w_all.append(result(0, moved, half))
        m_all.append(jacobi[half] * w_all[half])
        window[half] = m_all[half]
    w, m = middle_of(w_all), middle_of(m_all)

    def dots_1():
        g_row = rows[...]
        return start_plane(
            1, packed([dot(w, u), dot(w, m), total(a_row * g_row), total(g_row * g_row)])
        )

    reducing = start_depth(0, reducing)
    moved, later = applied(1, dots_1)
    g_row = rows[...]
    rho, norm = finish_depth(0, reducing, 2)
    reducing = start_depth(1, later)
    alpha = rho / norm
    z_all = []
    for half in range(2):
        z_all.append(result(1, moved, half))
        w_all[half] = w_all[half] - alpha * z_all[half]
        window[half] = jacobi[half] * w_all[half]
        m_all[half] = jacobi[half] * w_all[half]
    q, s, p = m, w, u
    ap_row, aq_row = a_row, g_row
    x = [alpha * one for one in p]
    u = [one - alpha * other for one, other in zip(u, q)]
    r = [one - alpha * other for one, other in zip(r, s)]
    residual = residual - alpha * ap_row
    a_row = a_row - alpha * aq_row
    w, m = middle_of(w_all), middle_of(m_all)
    old_rho, old_norm, old_alpha = rho, norm, alpha

    moved, _ = applied(2, None)
    g_row = rows[...]
    w_u, w_m, a_g, g_g = finish_depth(1, reducing, 4)
    rho = old_rho - 2.0 * old_alpha * w_u + old_alpha * old_alpha * w_m
    beta = rho / old_rho
    lead = 1.0 + beta
    norm = (
        lead * lead * old_norm
        - 2.0 * lead * old_alpha * a_g
        + old_alpha * old_alpha * g_g
    )
    alpha = rho / norm
    for half in range(2):
        z_all[half] = result(2, moved, half) + beta * z_all[half]
        w_all[half] = w_all[half] - alpha * z_all[half]
        window[half] = jacobi[half] * w_all[half]
    q = [one + beta * other for one, other in zip(m, q)]
    s = [one + beta * other for one, other in zip(w, s)]
    p = [one + beta * other for one, other in zip(u, p)]
    x = [one + alpha * other for one, other in zip(x, p)]
    r = [one - alpha * other for one, other in zip(r, s)]
    u = [one - alpha * other for one, other in zip(u, q)]
    ap_row = a_row + beta * ap_row
    aq_row = g_row + beta * aq_row
    residual = residual - alpha * ap_row
    a_row = a_row - alpha * aq_row
    w = middle_of(w_all)
    m = [window[half, pl.ds(nodes, nodes)] for half in range(2)]
    rho_1, norm_1 = rho, norm

    node_dots = [
        dot(r, u),
        dot(w, u),
        dot(w, p),
        dot(s, u),
        dot(w, m),
        dot(s, m),
        dot(s, q),
    ]

    @pl.loop(0, tiles, unroll=4)
    def _(tile):
        image_of(tile)

    g_row = rows[...]
    fields = [a_row, g_row, aq_row, ap_row]
    pairs = [(i, j) for i in range(4) for j in range(i, 4)]
    row_dots = [total(fields[i] * fields[j]) for i, j in pairs]
    later = start_depth(2, start_plane(2, packed(node_dots + row_dots)))
    found = finish_depth(2, later, len(node_dots) + len(pairs))
    rho_2, uu, cross, s_u, w_m, s_m, s_q = found[: len(node_dots)]
    gram = dict(zip(pairs, found[len(node_dots) :]))
    beta = rho_2 / rho_1
    norm_2 = uu + 2.0 * beta * cross + beta * beta * norm_1
    alpha = rho_2 / norm_2
    rho_3 = (
        rho_2
        - 2.0 * alpha * (uu + beta * s_u)
        + alpha * alpha * (w_m + 2.0 * beta * s_m + beta * beta * s_q)
    )
    beta_3 = rho_3 / rho_2
    weights = [1.0 + beta_3, -alpha, -alpha * beta, beta_3 * beta]
    norm_3 = 0.0
    for i, j in pairs:
        norm_3 = norm_3 + (1.0 if i == j else 2.0) * weights[i] * weights[j] * gram[i, j]
    alpha_3 = rho_3 / norm_3
    p = [one + beta * other for one, other in zip(u, p)]
    x = [one + alpha * other for one, other in zip(x, p)]
    u = [one - alpha * (other + beta * last) for one, other, last in zip(u, m, q)]
    p = [one + beta_3 * other for one, other in zip(u, p)]
    x = [one + alpha_3 * other for one, other in zip(x, p)]
    ap_row = a_row + beta * ap_row
    last_row = sum(weights[i] * fields[i] for i in range(4))
    residual_ref[...] = residual - alpha * ap_row - alpha_3 * last_row
    for half in range(2):
        mine = x[half][:NODES]
        for index in range(1, subs):
            mine = jnp.where(sub == index, x[half][index * NODES : (index + 1) * NODES], mine)
        solution_ref[:, 128 * half : 128 * (half + 1)] = mine
    for item in sent:
        item.wait_send()


def per_device(slabs, subs, values, block_ids, tile_counts, right_side):
    tiles, coupled, height, width = values.shape
    own = 2 * tiles
    nodes = subs * NODES
    along_x = min(ALONG_X, slabs // CORES)
    plane_count = along_x * subs
    depth_count = slabs // along_x
    half = width // 2
    vmem = pltpu.VMEM
    dma = pltpu.SemaphoreType.DMA
    return pl.pallas_call(
        functools.partial(kernel, slabs, subs, along_x),
        out_shape=(
            jax.ShapeDtypeStruct((NODES, width), F32),
            jax.ShapeDtypeStruct((tiles, height), F32),
        ),
        in_specs=[
            pl.BlockSpec(memory_space=pl.ANY),
            pl.BlockSpec(memory_space=pltpu.SMEM),
            pl.BlockSpec(memory_space=pl.ANY),
            pl.BlockSpec(memory_space=pl.ANY),
        ],
        out_specs=(
            pl.BlockSpec(memory_space=pltpu.VMEM),
            pl.BlockSpec(memory_space=pltpu.VMEM),
        ),
        scratch_shapes=[
            vmem(values.shape, F32),
            vmem((tiles, height), F32),
            pltpu.SMEM((2, tiles), jnp.int32),
            vmem((tiles, height, half), F32),
            vmem((subs, 1, 256), jnp.int32),
            vmem((2, 2, subs * own, half), F32),
            vmem((3, 2, 1, subs * own, half), F32),
            vmem((2, 2, 3 * nodes, half), F32),
            vmem((3, 2, 1, 3 * nodes, half), F32),
            vmem((2, 2, 2, 2 * nodes, half), F32),
            vmem((2, 2, 2, nodes, half), F32),
            vmem((3, 2, 2, 1, 2 * nodes, half), F32),
            vmem((3, 2, 2, 1, nodes, half), F32),
            vmem((2, 3 * nodes, half), F32),
            vmem((tiles, height), F32),
            vmem((3, plane_count, 1, 128), F32),
            vmem((3, depth_count, 1, 128), F32),
            dma((2 * GROUPS,)),
            dma,
            dma,
            dma((subs,)),
            dma((subs,)),
            dma((4, 2, subs)),
            dma((4, 2, subs)),
            dma((4, 2, 4)),
            dma((4, 2, 4)),
            dma((3, plane_count)),
            dma((3, plane_count)),
            dma((3, depth_count)),
            dma((3, depth_count)),
        ],
        compiler_params=pltpu.CompilerParams(
            collective_id=0, has_side_effects=True, vmem_limit_bytes=67043328
        ),
        name="cgls",
    )(block_ids.T, tile_counts, values, right_side)


def solution(mesh):
    both = ("slab", "sub")
    return jax.shard_map(
        functools.partial(per_device, mesh.shape["slab"], mesh.shape["sub"]),
        mesh=mesh,
        in_specs=(P(both, None, None, None), P(both, None), P("slab", "sub"), P(both, None)),
        out_specs=(P(both, None), P(both, None)),
        check_vma=False,
    )
```

```python
import functools

import jax
import jax.numpy as jnp
from jax import lax
from jax.experimental import pallas as pl
from jax.experimental.pallas import tpu as pltpu
from jax.sharding import PartitionSpec as P

MESH = pl.DeviceIdType.MESH
NODES = 12
CORES = 2
ALONG_X = 4
GROUPS = 3
F32 = jnp.float32
BF16 = jnp.bfloat16


def total(value):
    return jnp.sum(jnp.sum(value, axis=1, keepdims=True), axis=0, keepdims=True)


def packed(parts):
    lanes = lax.broadcasted_iota(jnp.int32, (1, 128), 1)
    row = jnp.zeros((1, 128), F32)
    for place, part in enumerate(parts):
        row = jnp.where(lanes == place, part, row)
    return row


def unpacked(row, count):
    lanes = lax.broadcasted_iota(jnp.int32, (1, 128), 1)
    return [
        jnp.sum(jnp.where(lanes == place, row, 0.0), axis=1, keepdims=True) for place in range(count)
    ]


def kernel(
    slabs,
    subs,
    along_x,
    ids_ref,
    count_ref,
    values_hbm,
    side,
    solution_ref,
    residual_ref,
    values,
    columns,
    ids_buf,
    terms,
    sums,
    near,
    far,
    window,
    rows,
    plane,
    depth,
    load_sem,
    ids_send,
    ids_recv,
    term_send,
    term_recv,
    sum_send,
    sum_recv,
    plane_send,
    plane_recv,
    depth_send,
    depth_recv,
):
    tiles = values.shape[0]
    own = 2 * tiles
    nodes = subs * NODES
    slab = lax.axis_index("slab")
    sub = lax.axis_index("sub")
    along_z = slabs // (along_x * CORES)
    core = lax.rem(slab, CORES)
    x_at = lax.rem(slab // CORES, along_x)
    z_at = slab // (CORES * along_x)
    plane_count = along_x * subs
    depth_count = along_z * CORES
    plane_at = x_at * subs + sub
    depth_at = z_at * CORES + core

    def sub_peer(step):
        return (slab, lax.rem(sub + step, subs))

    def slab_peer(step):
        return (lax.rem(slab + step + slabs, slabs), sub)

    def plane_peer(step):
        at = lax.rem(plane_at + step, plane_count)
        return ((z_at * along_x + at // subs) * CORES + core, lax.rem(at, subs))

    def depth_peer(step):
        at = lax.rem(depth_at + step, depth_count)
        return ((at // CORES * along_x + x_at) * CORES + lax.rem(at, CORES), sub)

    def half_of(half):
        return pl.ds(128 * half, 128)

    group = tiles // GROUPS
    loads = []
    for half in range(2):
        for part in range(GROUPS):
            at = (pl.ds(part * group, group), slice(None), slice(None), half_of(half))
            loads.append(
                pltpu.make_async_copy(
                    values_hbm.at[at], values.at[at], load_sem.at[half * GROUPS + part]
                )
            )
    for load in loads:
        load.start()

    barrier = pltpu.get_barrier_semaphore()
    partners = (
        [slab_peer(step) for step in (-2, -1, 1, 2)]
        + [plane_peer(step) for step in range(1, plane_count)]
        + [depth_peer(step) for step in range(1, depth_count)]
    )
    for partner in partners:
        pl.semaphore_signal(barrier, inc=1, device_id=partner, device_id_type=MESH)

    base = (slab - 1) * nodes
    count = count_ref[0, 0]
    lanes = lax.broadcasted_iota(jnp.int32, (1, 256), 1)
    ids_row = jnp.zeros((1, 256), jnp.int32)
    for tile in range(tiles):
        for slot in range(2):
            mark = ids_ref[slot, tile] - base + 1
            ids_row = jnp.where(lanes == sub * own + 2 * tile + slot, mark, ids_row)
    ids_buf[sub] = ids_row

    live_rows = lax.broadcasted_iota(jnp.int32, (tiles, 128), 0) < count
    residual = jnp.where(live_rows, side[...], 0.0)
    rows[...] = residual
    eye = lax.broadcasted_iota(jnp.int32, (128, 128), 0) == lax.broadcasted_iota(
        jnp.int32, (128, 128), 1
    )
    sent = []

    def copy(source, target, send, recv, peer):
        item = pltpu.make_async_remote_copy(
            src_ref=source,
            dst_ref=target,
            send_sem=send,
            recv_sem=recv,
            device_id=peer,
            device_id_type=MESH,
        )
        item.start()
        sent.append(item)
        return item

    def live_of(tile):
        return jnp.where(tile < count, 1.0, 0.0).astype(F32)

    def place_of(tile, slot):
        return pl.ds(sub * own + 2 * tile + slot, 1)

    def first_tile(tile, half):
        live = live_of(tile)
        if half == 0:
            column = jnp.sum(
                jnp.where(eye, rows[pl.ds(tile, 1), :], 0.0), axis=1, keepdims=True
            )
            column = jnp.broadcast_to(column, (128, 128))
            columns[tile] = column
        else:
            column = columns[tile]
        for slot in range(2):
            block = values[tile, slot, :, 128 * half : 128 * (half + 1)]
            at = place_of(tile, slot)
            terms[0, half, at, :] = jnp.sum(block * column, axis=0, keepdims=True)
            terms[1, half, at, :] = jnp.sum(block * block, axis=0, keepdims=True) * live

    def image_of(tile):
        live = live_of(tile)
        product = None
        for slot in range(2):
            at = jnp.minimum(jnp.maximum(ids_ref[slot, tile] - base, 0), 3 * nodes - 1)
            for half in range(2):
                row = window[half, pl.ds(at, 1), :] * live
                part = values[tile, slot, :, 128 * half : 128 * (half + 1)] * row
                product = part if product is None else product + part
        column = jnp.sum(product, axis=1, keepdims=True)
        rows[pl.ds(tile, 1), :] = jnp.sum(jnp.where(eye, column, 0.0), axis=0, keepdims=True)
        return column

    def back_tile(phase, tile, half):
        if half == 0:
            column = jnp.broadcast_to(image_of(tile), (128, 128))
            columns[tile] = column
        else:
            column = columns[tile]
        for slot in range(2):
            block = values[tile, slot, :, 128 * half : 128 * (half + 1)]
            terms[phase, half, place_of(tile, slot), :] = jnp.sum(
                block * column, axis=0, keepdims=True
            )

    def spread(phase, half, part):
        at = terms.at[phase, half, pl.ds(sub * own + 2 * part * group, 2 * group)]
        return [
            copy(
                at,
                at,
                term_send.at[phase, half, part, step],
                term_recv.at[phase, half, part, step],
                sub_peer(step),
            )
            for step in sorted(range(1, subs), key=lambda step: -min(step, subs - step))
        ]

    def arrived(items):
        for item in items:
            item.wait_recv()

    def summed(value):
        high = value.astype(BF16)
        rest = value - high.astype(F32)
        middle = rest.astype(BF16)
        low = (rest - middle.astype(F32)).astype(BF16)
        return sum(
            jnp.dot(selector, piece, preferred_element_type=F32) for piece in (high, middle, low)
        )

    def exchange(phase, half):
        mine = summed(terms[phase, half])
        sums[phase, half] = mine
        moves = (
            (2, pl.ds(2 * nodes, nodes), far.at[phase, half, 0]),
            (-2, pl.ds(0, nodes), far.at[phase, half, 1]),
            (1, pl.ds(nodes, 2 * nodes), near.at[phase, half, 0]),
            (-1, pl.ds(0, 2 * nodes), near.at[phase, half, 1]),
        )
        items = [
            copy(
                sums.at[phase, half, part],
                target,
                sum_send.at[phase, half, place],
                sum_recv.at[phase, half, place],
                slab_peer(step),
            )
            for place, (step, part, target) in enumerate(moves)
        ]
        return mine, items

    def result(phase, half, moved):
        value, items = moved
        arrived(items)
        below, above = near[phase, half, 0], near[phase, half, 1]
        return jnp.concatenate(
            [
                (far[phase, half, 0] + below[:nodes]) + value[:nodes],
                (below[nodes:] + value[nodes : 2 * nodes]) + above[:nodes],
                (value[2 * nodes :] + above[nodes:]) + far[phase, half, 1],
            ],
            axis=0,
        )

    def start_plane(index, row):
        plane[index, plane_at] = row
        at = plane.at[index, plane_at]
        return [
            copy(at, at, plane_send.at[index, step], plane_recv.at[index, step], plane_peer(step))
            for step in range(1, plane_count)
        ]

    def start_depth(index, items):
        arrived(items)
        depth[index, depth_at] = jnp.sum(plane[index], axis=0)
        at = depth.at[index, depth_at]
        return [
            copy(at, at, depth_send.at[index, step], depth_recv.at[index, step], depth_peer(step))
            for step in range(1, depth_count)
        ]

    def finish_depth(index, items, number):
        arrived(items)
        return unpacked(jnp.sum(depth[index], axis=0), number)

    def middle_of(halves):
        return [half[nodes : 2 * nodes] for half in halves]

    def dot(one, other):
        return total(one[0] * other[0] + one[1] * other[1]) * (1.0 / subs)

    items = {(phase, half): [] for phase in range(2) for half in range(2)}
    for half in range(2):
        for part in range(GROUPS):
            loads[half * GROUPS + part].wait()

            @pl.loop(part * group, (part + 1) * group, unroll=4)
            def _(tile):
                first_tile(tile, half)

            if half == 0 and part == 0:
                pl.semaphore_wait(barrier, len(partners))
                place = ids_buf.at[sub]
                ids_items = [
                    copy(place, place, ids_send.at[step], ids_recv.at[step], sub_peer(step))
                    for step in range(1, subs)
                ]
            for phase in range(2):
                items[phase, half] += spread(phase, half, part)
    arrived(ids_items)
    all_ids = sum(ids_buf[i] for i in range(subs))[:, : subs * own]
    row_ids = lax.broadcasted_iota(jnp.int32, (3 * nodes, subs * own), 0) + 1
    selector = jnp.where(row_ids == all_ids, 1.0, 0.0).astype(BF16)
    moved = {}
    for half in range(2):
        for phase in range(2):
            arrived(items[phase, half])
            moved[phase, half] = exchange(phase, half)
    normal, jacobi, u_all = [], [], []
    for half in range(2):
        normal.append(result(0, half, moved[0, half]))
        jacobi.append(1.0 / (1.0 + result(1, half, moved[1, half])))
        u_all.append(jacobi[half] * normal[half])
        window[half] = u_all[half]

    def applied(phase, meanwhile):
        items = [[], []]
        for half in range(2):
            for part in range(GROUPS):

                @pl.loop(part * group, (part + 1) * group, unroll=4)
                def _(tile):
                    back_tile(phase, tile, half)

                items[half] += spread(phase, half, part)
        found = meanwhile()
        moved = []
        for half in range(2):
            arrived(items[half])
            moved.append(exchange(phase, half))
        return moved, found

    r, u = middle_of(normal), middle_of(u_all)

    def beside_0():
        a_row = rows[...]
        return start_plane(0, packed([dot(r, u), total(a_row * a_row)])), a_row

    moved, (reducing, a_row) = applied(2, beside_0)
    w_all, m_all = [], []
    for half in range(2):
        w_all.append(result(2, half, moved[half]))
        m_all.append(jacobi[half] * w_all[half])
        window[half] = m_all[half]

    w, m = middle_of(w_all), middle_of(m_all)

    def beside_1():
        g_row = rows[...]
        later = start_plane(
            1, packed([dot(w, u), dot(w, m), total(a_row * g_row), total(g_row * g_row)])
        )
        return start_depth(0, reducing), later, g_row

    moved, (reducing, later, g_row) = applied(3, beside_1)
    rho, norm = finish_depth(0, reducing, 2)
    reducing = start_depth(1, later)
    alpha = rho / norm
    z_all = []
    for half in range(2):
        z_all.append(result(3, half, moved[half]))
        w_all[half] = w_all[half] - alpha * z_all[half]
        window[half] = jacobi[half] * w_all[half]
    old_rho, old_norm, old_alpha = rho, norm, alpha

    def beside_2():
        q, s, p = m, w, u
        x = [old_alpha * one for one in p]
        new_u = [one - old_alpha * other for one, other in zip(u, q)]
        new_r = [one - old_alpha * other for one, other in zip(r, s)]
        new_residual = residual - old_alpha * a_row
        new_a = a_row - old_alpha * g_row
        new_w = middle_of(w_all)
        new_m = [jacobi[half][nodes : 2 * nodes] * new_w[half] for half in range(2)]
        return q, s, p, x, new_u, new_r, new_residual, new_a, new_w, new_m, rows[...]

    moved, kept = applied(4, beside_2)
    ap_row, aq_row = a_row, g_row
    q, s, p, x, u, r, residual, a_row, w, m, g_row = kept
    w_u, w_m, a_g, g_g = finish_depth(1, reducing, 4)
    rho = old_rho - 2.0 * old_alpha * w_u + old_alpha * old_alpha * w_m
    beta = rho / old_rho
    lead = 1.0 + beta
    norm = (
        lead * lead * old_norm
        - 2.0 * lead * old_alpha * a_g
        + old_alpha * old_alpha * g_g
    )
    alpha = rho / norm
    q = [one + beta * other for one, other in zip(m, q)]
    s = [one + beta * other for one, other in zip(w, s)]
    p = [one + beta * other for one, other in zip(u, p)]
    x = [one + alpha * other for one, other in zip(x, p)]
    r = [one - alpha * other for one, other in zip(r, s)]
    u = [one - alpha * other for one, other in zip(u, q)]
    ap_row = a_row + beta * ap_row
    aq_row = g_row + beta * aq_row
    residual = residual - alpha * ap_row
    a_row = a_row - alpha * aq_row
    for half in range(2):
        z_all[half] = result(4, half, moved[half]) + beta * z_all[half]
        w_all[half] = w_all[half] - alpha * z_all[half]
        window[half] = jacobi[half] * w_all[half]
    w = middle_of(w_all)
    m = [window[half, pl.ds(nodes, nodes)] for half in range(2)]
    rho_1, norm_1 = rho, norm

    node_dots = [
        dot(r, u),
        dot(w, u),
        dot(w, p),
        dot(s, u),
        dot(w, m),
        dot(s, m),
        dot(s, q),
    ]

    @pl.loop(0, tiles, unroll=4)
    def _(tile):
        image_of(tile)

    g_row = rows[...]
    fields = [a_row, g_row, aq_row, ap_row]
    pairs = [(i, j) for i in range(4) for j in range(i, 4)]
    row_dots = [total(fields[i] * fields[j]) for i, j in pairs]
    later = start_depth(2, start_plane(2, packed(node_dots + row_dots)))
    found = finish_depth(2, later, len(node_dots) + len(pairs))
    rho_2, uu, cross, s_u, w_m, s_m, s_q = found[: len(node_dots)]
    gram = dict(zip(pairs, found[len(node_dots) :]))
    beta = rho_2 / rho_1
    norm_2 = uu + 2.0 * beta * cross + beta * beta * norm_1
    alpha = rho_2 / norm_2
    rho_3 = (
        rho_2
        - 2.0 * alpha * (uu + beta * s_u)
        + alpha * alpha * (w_m + 2.0 * beta * s_m + beta * beta * s_q)
    )
    beta_3 = rho_3 / rho_2
    weights = [1.0 + beta_3, -alpha, -alpha * beta, beta_3 * beta]
    norm_3 = 0.0
    for i, j in pairs:
        norm_3 = norm_3 + (1.0 if i == j else 2.0) * weights[i] * weights[j] * gram[i, j]
    alpha_3 = rho_3 / norm_3
    p = [one + beta * other for one, other in zip(u, p)]
    x = [one + alpha * other for one, other in zip(x, p)]
    u = [one - alpha * (other + beta * last) for one, other, last in zip(u, m, q)]
    p = [one + beta_3 * other for one, other in zip(u, p)]
    x = [one + alpha_3 * other for one, other in zip(x, p)]
    ap_row = a_row + beta * ap_row
    last_row = sum(weights[i] * fields[i] for i in range(4))
    residual_ref[...] = residual - alpha * ap_row - alpha_3 * last_row
    for half in range(2):
        mine = x[half][:NODES]
        for index in range(1, subs):
            mine = jnp.where(sub == index, x[half][index * NODES : (index + 1) * NODES], mine)
        solution_ref[:, 128 * half : 128 * (half + 1)] = mine
    for item in sent:
        item.wait_send()


def per_device(slabs, subs, values, block_ids, tile_counts, right_side):
    tiles, coupled, height, width = values.shape
    own = 2 * tiles
    nodes = subs * NODES
    along_x = min(ALONG_X, slabs // CORES)
    plane_count = along_x * subs
    depth_count = slabs // along_x
    half = width // 2
    vmem = pltpu.VMEM
    dma = pltpu.SemaphoreType.DMA
    return pl.pallas_call(
        functools.partial(kernel, slabs, subs, along_x),
        out_shape=(
            jax.ShapeDtypeStruct((NODES, width), F32),
            jax.ShapeDtypeStruct((tiles, height), F32),
        ),
        in_specs=[
            pl.BlockSpec(memory_space=pltpu.SMEM),
            pl.BlockSpec(memory_space=pltpu.SMEM),
            pl.BlockSpec(memory_space=pl.ANY),
            pl.BlockSpec(memory_space=pltpu.VMEM),
        ],
        out_specs=(
            pl.BlockSpec(memory_space=pltpu.VMEM),
            pl.BlockSpec(memory_space=pltpu.VMEM),
        ),
        scratch_shapes=[
            vmem(values.shape, F32),
            vmem((tiles, height, half), F32),
            vmem((subs, 1, 256), jnp.int32),
            vmem((5, 2, subs * own, half), F32),
            vmem((5, 2, 3 * nodes, half), F32),
            vmem((5, 2, 2, 2 * nodes, half), F32),
            vmem((5, 2, 2, nodes, half), F32),
            vmem((2, 3 * nodes, half), F32),
            vmem((tiles, height), F32),
            vmem((3, plane_count, 1, 128), F32),
            vmem((3, depth_count, 1, 128), F32),
            dma((2 * GROUPS,)),
            dma((subs,)),
            dma((subs,)),
            dma((5, 2, GROUPS, subs)),
            dma((5, 2, GROUPS, subs)),
            dma((5, 2, 4)),
            dma((5, 2, 4)),
            dma((3, plane_count)),
            dma((3, plane_count)),
            dma((3, depth_count)),
            dma((3, depth_count)),
        ],
        compiler_params=pltpu.CompilerParams(
            collective_id=0, has_side_effects=True, vmem_limit_bytes=48 * 1024 * 1024
        ),
        name="cgls",
    )(block_ids.T, tile_counts, values, right_side)


def solution(mesh):
    both = ("slab", "sub")
    return jax.shard_map(
        functools.partial(per_device, mesh.shape["slab"], mesh.shape["sub"]),
        mesh=mesh,
        in_specs=(P(both, None, None, None), P(both, None), P("slab", "sub"), P(both, None)),
        out_specs=(P(both, None), P(both, None)),
        check_vma=False,
    )
```

```python
import functools

import jax
import jax.numpy as jnp
from jax import lax
from jax.experimental import pallas as pl
from jax.experimental.pallas import tpu as pltpu
from jax.sharding import PartitionSpec as P

MESH = pl.DeviceIdType.MESH
NODES = 12
CORES = 2
ALONG_X = 4
GROUPS = 1
LOADS = 3
F32 = jnp.float32
BF16 = jnp.bfloat16


def total(value):
    return jnp.sum(jnp.sum(value, axis=1, keepdims=True), axis=0, keepdims=True)


def packed(parts):
    lanes = lax.broadcasted_iota(jnp.int32, (1, 128), 1)
    row = jnp.zeros((1, 128), F32)
    for place, part in enumerate(parts):
        row = jnp.where(lanes == place, part, row)
    return row


def unpacked(row, count):
    lanes = lax.broadcasted_iota(jnp.int32, (1, 128), 1)
    return [
        jnp.sum(jnp.where(lanes == place, row, 0.0), axis=1, keepdims=True) for place in range(count)
    ]


def kernel(
    slabs,
    subs,
    along_x,
    ids_ref,
    count_ref,
    values_hbm,
    side,
    solution_ref,
    residual_ref,
    values,
    columns,
    ids_buf,
    terms,
    sums,
    near,
    far,
    window,
    rows,
    plane,
    depth,
    load_sem,
    ids_send,
    ids_recv,
    term_send,
    term_recv,
    sum_send,
    sum_recv,
    plane_send,
    plane_recv,
    depth_send,
    depth_recv,
):
    tiles = values.shape[0]
    own = 2 * tiles
    nodes = subs * NODES
    slab = lax.axis_index("slab")
    sub = lax.axis_index("sub")
    along_z = slabs // (along_x * CORES)
    core = lax.rem(slab, CORES)
    x_at = lax.rem(slab // CORES, along_x)
    z_at = slab // (CORES * along_x)
    plane_count = along_x * subs
    depth_count = along_z * CORES
    plane_at = x_at * subs + sub
    depth_at = z_at * CORES + core

    def sub_peer(step):
        return (slab, lax.rem(sub + step, subs))

    def slab_peer(step):
        return (lax.rem(slab + step + slabs, slabs), sub)

    def plane_peer(step):
        at = lax.rem(plane_at + step, plane_count)
        return ((z_at * along_x + at // subs) * CORES + core, lax.rem(at, subs))

    def depth_peer(step):
        at = lax.rem(depth_at + step, depth_count)
        return ((at // CORES * along_x + x_at) * CORES + lax.rem(at, CORES), sub)

    def half_of(half):
        return pl.ds(128 * half, 128)

    group = tiles // GROUPS
    share = tiles // LOADS
    loads = []
    for half in range(2):
        for part in range(LOADS):
            at = (pl.ds(part * share, share), slice(None), slice(None), half_of(half))
            loads.append(
                pltpu.make_async_copy(
                    values_hbm.at[at], values.at[at], load_sem.at[half * LOADS + part]
                )
            )
    for load in loads:
        load.start()

    barrier = pltpu.get_barrier_semaphore()
    partners = (
        [slab_peer(step) for step in (-2, -1, 1, 2)]
        + [plane_peer(step) for step in range(1, plane_count)]
        + [depth_peer(step) for step in range(1, depth_count)]
    )
    for partner in partners:
        pl.semaphore_signal(barrier, inc=1, device_id=partner, device_id_type=MESH)

    base = (slab - 1) * nodes
    count = count_ref[0, 0]
    lanes = lax.broadcasted_iota(jnp.int32, (1, 256), 1)
    ids_row = jnp.zeros((1, 256), jnp.int32)
    for tile in range(tiles):
        for slot in range(2):
            mark = ids_ref[slot, tile] - base + 1
            ids_row = jnp.where(lanes == sub * own + 2 * tile + slot, mark, ids_row)
    ids_buf[sub] = ids_row

    live_rows = lax.broadcasted_iota(jnp.int32, (tiles, 128), 0) < count
    residual = jnp.where(live_rows, side[...], 0.0)
    rows[...] = residual
    eye = lax.broadcasted_iota(jnp.int32, (128, 128), 0) == lax.broadcasted_iota(
        jnp.int32, (128, 128), 1
    )
    sent = []

    def copy(source, target, send, recv, peer):
        item = pltpu.make_async_remote_copy(
            src_ref=source,
            dst_ref=target,
            send_sem=send,
            recv_sem=recv,
            device_id=peer,
            device_id_type=MESH,
        )
        item.start()
        sent.append(item)
        return item

    def live_of(tile):
        return jnp.where(tile < count, 1.0, 0.0).astype(F32)

    def place_of(tile, slot):
        return pl.ds(sub * own + 2 * tile + slot, 1)

    def first_tile(tile, half):
        live = live_of(tile)
        if half == 0:
            column = jnp.sum(
                jnp.where(eye, rows[pl.ds(tile, 1), :], 0.0), axis=1, keepdims=True
            )
            column = jnp.broadcast_to(column, (128, 128))
            columns[tile] = column
        else:
            column = columns[tile]
        for slot in range(2):
            block = values[tile, slot, :, 128 * half : 128 * (half + 1)]
            at = place_of(tile, slot)
            terms[0, half, at, :] = jnp.sum(block * column, axis=0, keepdims=True)
            terms[1, half, at, :] = jnp.sum(block * block, axis=0, keepdims=True) * live

    def picked(tile, half):
        live = live_of(tile)
        product = None
        for slot in range(2):
            at = jnp.minimum(jnp.maximum(ids_ref[slot, tile] - base, 0), 3 * nodes - 1)
            row = window[half, pl.ds(at, 1), :] * live
            part = values[tile, slot, :, 128 * half : 128 * (half + 1)] * row
            product = part if product is None else product + part
        return product

    def begin_images():
        @pl.loop(0, tiles, unroll=8)
        def _(tile):
            columns[tile] = picked(tile, 0)

    def image_of(tile):
        column = jnp.sum(columns[tile] + picked(tile, 1), axis=1, keepdims=True)
        rows[pl.ds(tile, 1), :] = jnp.sum(jnp.where(eye, column, 0.0), axis=0, keepdims=True)
        return column

    def back_tile(phase, tile, half):
        if half == 0:
            column = jnp.broadcast_to(image_of(tile), (128, 128))
            columns[tile] = column
        else:
            column = columns[tile]
        for slot in range(2):
            block = values[tile, slot, :, 128 * half : 128 * (half + 1)]
            terms[phase, half, place_of(tile, slot), :] = jnp.sum(
                block * column, axis=0, keepdims=True
            )

    def spread(phase, half, part):
        at = terms.at[phase, half, pl.ds(sub * own + 2 * part * group, 2 * group)]
        return [
            copy(
                at,
                at,
                term_send.at[phase, half, part, step],
                term_recv.at[phase, half, part, step],
                sub_peer(step),
            )
            for step in sorted(range(1, subs), key=lambda step: -min(step, subs - step))
        ]

    def arrived(items):
        for item in items:
            item.wait_recv()

    def summed(value):
        high = value.astype(BF16)
        rest = value - high.astype(F32)
        middle = rest.astype(BF16)
        low = (rest - middle.astype(F32)).astype(BF16)
        return sum(
            jnp.dot(selector, piece, preferred_element_type=F32) for piece in (high, middle, low)
        )

    def exchange(phase, half):
        mine = summed(terms[phase, half])
        sums[phase, half] = mine
        moves = (
            (2, pl.ds(2 * nodes, nodes), far.at[phase, half, 0]),
            (-2, pl.ds(0, nodes), far.at[phase, half, 1]),
            (1, pl.ds(nodes, 2 * nodes), near.at[phase, half, 0]),
            (-1, pl.ds(0, 2 * nodes), near.at[phase, half, 1]),
        )
        items = [
            copy(
                sums.at[phase, half, part],
                target,
                sum_send.at[phase, half, place],
                sum_recv.at[phase, half, place],
                slab_peer(step),
            )
            for place, (step, part, target) in enumerate(moves)
        ]
        return mine, items

    def result(phase, half, moved):
        value, items = moved
        arrived(items)
        below, above = near[phase, half, 0], near[phase, half, 1]
        return jnp.concatenate(
            [
                (far[phase, half, 0] + below[:nodes]) + value[:nodes],
                (below[nodes:] + value[nodes : 2 * nodes]) + above[:nodes],
                (value[2 * nodes :] + above[nodes:]) + far[phase, half, 1],
            ],
            axis=0,
        )

    def start_plane(index, row):
        plane[index, plane_at] = row
        at = plane.at[index, plane_at]
        return [
            copy(at, at, plane_send.at[index, step], plane_recv.at[index, step], plane_peer(step))
            for step in range(1, plane_count)
        ]

    def start_depth(index, items):
        arrived(items)
        depth[index, depth_at] = jnp.sum(plane[index], axis=0)
        at = depth.at[index, depth_at]
        return [
            copy(at, at, depth_send.at[index, step], depth_recv.at[index, step], depth_peer(step))
            for step in range(1, depth_count)
        ]

    def finish_depth(index, items, number):
        arrived(items)
        return unpacked(jnp.sum(depth[index], axis=0), number)

    def middle_of(halves):
        return [half[nodes : 2 * nodes] for half in halves]

    def dot(one, other):
        return total(one[0] * other[0] + one[1] * other[1]) * (1.0 / subs)

    items = {(phase, half): [] for phase in range(2) for half in range(2)}
    for half in range(2):
        for part in range(LOADS):
            loads[half * LOADS + part].wait()

            @pl.loop(part * share, (part + 1) * share, unroll=4)
            def _(tile):
                first_tile(tile, half)

        if half == 0:
            pl.semaphore_wait(barrier, len(partners))
            place = ids_buf.at[sub]
            ids_items = [
                copy(place, place, ids_send.at[step], ids_recv.at[step], sub_peer(step))
                for step in range(1, subs)
            ]
        for phase in range(2):
            items[phase, half] += spread(phase, half, 0)
    arrived(ids_items)
    all_ids = sum(ids_buf[i] for i in range(subs))[:, : subs * own]
    row_ids = lax.broadcasted_iota(jnp.int32, (3 * nodes, subs * own), 0) + 1
    selector = jnp.where(row_ids == all_ids, 1.0, 0.0).astype(BF16)
    moved = {}
    for half in range(2):
        for phase in range(2):
            arrived(items[phase, half])
            moved[phase, half] = exchange(phase, half)
    normal, jacobi, u_all = [], [], []
    for half in range(2):
        normal.append(result(0, half, moved[0, half]))
        jacobi.append(1.0 / (1.0 + result(1, half, moved[1, half])))
        u_all.append(jacobi[half] * normal[half])
        window[half] = u_all[half]
        if half == 0:
            begin_images()

    def applied(phase, meanwhile):
        items = [[], []]
        for half in range(2):
            for part in range(GROUPS):

                @pl.loop(part * group, (part + 1) * group, unroll=12)
                def _(tile):
                    back_tile(phase, tile, half)

                items[half] += spread(phase, half, part)
        found = meanwhile()
        moved = []
        for half in range(2):
            arrived(items[half])
            moved.append(exchange(phase, half))
        return moved, found

    r, u = middle_of(normal), middle_of(u_all)

    def beside_0():
        a_row = rows[...]
        return start_plane(0, packed([dot(r, u), total(a_row * a_row)])), a_row

    moved, (reducing, a_row) = applied(2, beside_0)
    w_all, m_all = [], []
    for half in range(2):
        w_all.append(result(2, half, moved[half]))
        m_all.append(jacobi[half] * w_all[half])
        window[half] = m_all[half]
        if half == 0:
            begin_images()

    w, m = middle_of(w_all), middle_of(m_all)

    def beside_1():
        g_row = rows[...]
        later = start_plane(
            1, packed([dot(w, u), dot(w, m), total(a_row * g_row), total(g_row * g_row)])
        )
        return start_depth(0, reducing), later, g_row

    moved, (reducing, later, g_row) = applied(3, beside_1)
    rho, norm = finish_depth(0, reducing, 2)
    reducing = start_depth(1, later)
    alpha = rho / norm
    z_all = []
    for half in range(2):
        z_all.append(result(3, half, moved[half]))
        w_all[half] = w_all[half] - alpha * z_all[half]
        window[half] = jacobi[half] * w_all[half]
        if half == 0:
            begin_images()
    old_rho, old_norm, old_alpha = rho, norm, alpha

    def beside_2():
        q, s, p = m, w, u
        x = [old_alpha * one for one in p]
        new_u = [one - old_alpha * other for one, other in zip(u, q)]
        new_r = [one - old_alpha * other for one, other in zip(r, s)]
        new_residual = residual - old_alpha * a_row
        new_a = a_row - old_alpha * g_row
        new_w = middle_of(w_all)
        new_m = [jacobi[half][nodes : 2 * nodes] * new_w[half] for half in range(2)]
        return q, s, p, x, new_u, new_r, new_residual, new_a, new_w, new_m, rows[...]

    moved, kept = applied(4, beside_2)
    ap_row, aq_row = a_row, g_row
    q, s, p, x, u, r, residual, a_row, w, m, g_row = kept
    w_u, w_m, a_g, g_g = finish_depth(1, reducing, 4)
    rho = old_rho - 2.0 * old_alpha * w_u + old_alpha * old_alpha * w_m
    beta = rho / old_rho
    lead = 1.0 + beta
    norm = (
        lead * lead * old_norm
        - 2.0 * lead * old_alpha * a_g
        + old_alpha * old_alpha * g_g
    )
    alpha = rho / norm
    q = [one + beta * other for one, other in zip(m, q)]
    s = [one + beta * other for one, other in zip(w, s)]
    p = [one + beta * other for one, other in zip(u, p)]
    x = [one + alpha * other for one, other in zip(x, p)]
    r = [one - alpha * other for one, other in zip(r, s)]
    u = [one - alpha * other for one, other in zip(u, q)]
    ap_row = a_row + beta * ap_row
    aq_row = g_row + beta * aq_row
    residual = residual - alpha * ap_row
    a_row = a_row - alpha * aq_row
    for half in range(2):
        z_all[half] = result(4, half, moved[half]) + beta * z_all[half]
        w_all[half] = w_all[half] - alpha * z_all[half]
        window[half] = jacobi[half] * w_all[half]
        if half == 0:
            begin_images()
    w = middle_of(w_all)
    m = [window[half, pl.ds(nodes, nodes)] for half in range(2)]
    rho_1, norm_1 = rho, norm

    node_dots = [
        dot(r, u),
        dot(w, u),
        dot(w, p),
        dot(s, u),
        dot(w, m),
        dot(s, m),
        dot(s, q),
    ]

    @pl.loop(0, tiles, unroll=4)
    def _(tile):
        image_of(tile)

    g_row = rows[...]
    fields = [a_row, g_row, aq_row, ap_row]
    pairs = [(i, j) for i in range(4) for j in range(i, 4)]
    row_dots = [total(fields[i] * fields[j]) for i, j in pairs]
    later = start_depth(2, start_plane(2, packed(node_dots + row_dots)))
    found = finish_depth(2, later, len(node_dots) + len(pairs))
    rho_2, uu, cross, s_u, w_m, s_m, s_q = found[: len(node_dots)]
    gram = dict(zip(pairs, found[len(node_dots) :]))
    beta = rho_2 / rho_1
    norm_2 = uu + 2.0 * beta * cross + beta * beta * norm_1
    alpha = rho_2 / norm_2
    rho_3 = (
        rho_2
        - 2.0 * alpha * (uu + beta * s_u)
        + alpha * alpha * (w_m + 2.0 * beta * s_m + beta * beta * s_q)
    )
    beta_3 = rho_3 / rho_2
    weights = [1.0 + beta_3, -alpha, -alpha * beta, beta_3 * beta]
    norm_3 = 0.0
    for i, j in pairs:
        norm_3 = norm_3 + (1.0 if i == j else 2.0) * weights[i] * weights[j] * gram[i, j]
    alpha_3 = rho_3 / norm_3
    p = [one + beta * other for one, other in zip(u, p)]
    x = [one + alpha * other for one, other in zip(x, p)]
    u = [one - alpha * (other + beta * last) for one, other, last in zip(u, m, q)]
    p = [one + beta_3 * other for one, other in zip(u, p)]
    x = [one + alpha_3 * other for one, other in zip(x, p)]
    ap_row = a_row + beta * ap_row
    last_row = sum(weights[i] * fields[i] for i in range(4))
    residual_ref[...] = residual - alpha * ap_row - alpha_3 * last_row
    for half in range(2):
        mine = x[half][:NODES]
        for index in range(1, subs):
            mine = jnp.where(sub == index, x[half][index * NODES : (index + 1) * NODES], mine)
        solution_ref[:, 128 * half : 128 * (half + 1)] = mine
    for item in sent:
        item.wait_send()


def per_device(slabs, subs, values, block_ids, tile_counts, right_side):
    tiles, coupled, height, width = values.shape
    own = 2 * tiles
    nodes = subs * NODES
    along_x = min(ALONG_X, slabs // CORES)
    plane_count = along_x * subs
    depth_count = slabs // along_x
    half = width // 2
    vmem = pltpu.VMEM
    dma = pltpu.SemaphoreType.DMA
    return pl.pallas_call(
        functools.partial(kernel, slabs, subs, along_x),
        out_shape=(
            jax.ShapeDtypeStruct((NODES, width), F32),
            jax.ShapeDtypeStruct((tiles, height), F32),
        ),
        in_specs=[
            pl.BlockSpec(memory_space=pltpu.SMEM),
            pl.BlockSpec(memory_space=pltpu.SMEM),
            pl.BlockSpec(memory_space=pl.ANY),
            pl.BlockSpec(memory_space=pltpu.VMEM),
        ],
        out_specs=(
            pl.BlockSpec(memory_space=pltpu.VMEM),
            pl.BlockSpec(memory_space=pltpu.VMEM),
        ),
        scratch_shapes=[
            vmem(values.shape, F32),
            vmem((tiles, height, half), F32),
            vmem((subs, 1, 256), jnp.int32),
            vmem((5, 2, subs * own, half), F32),
            vmem((5, 2, 3 * nodes, half), F32),
            vmem((5, 2, 2, 2 * nodes, half), F32),
            vmem((5, 2, 2, nodes, half), F32),
            vmem((2, 3 * nodes, half), F32),
            vmem((tiles, height), F32),
            vmem((3, plane_count, 1, 128), F32),
            vmem((3, depth_count, 1, 128), F32),
            dma((2 * LOADS,)),
            dma((subs,)),
            dma((subs,)),
            dma((5, 2, GROUPS, subs)),
            dma((5, 2, GROUPS, subs)),
            dma((5, 2, 4)),
            dma((5, 2, 4)),
            dma((3, plane_count)),
            dma((3, plane_count)),
            dma((3, depth_count)),
            dma((3, depth_count)),
        ],
        compiler_params=pltpu.CompilerParams(
            collective_id=0, has_side_effects=True, vmem_limit_bytes=48 * 1024 * 1024
        ),
        name="cgls",
    )(block_ids.T, tile_counts, values, right_side)


def solution(mesh):
    both = ("slab", "sub")
    return jax.shard_map(
        functools.partial(per_device, mesh.shape["slab"], mesh.shape["sub"]),
        mesh=mesh,
        in_specs=(P(both, None, None, None), P(both, None), P("slab", "sub"), P(both, None)),
        out_specs=(P(both, None), P(both, None)),
        check_vma=False,
    )
```

```python
import functools

import jax
import jax.numpy as jnp
from jax import lax
from jax.experimental import pallas as pl
from jax.experimental.pallas import tpu as pltpu
from jax.sharding import PartitionSpec as P

MESH = pl.DeviceIdType.MESH
NODES = 12
CORES = 2
ALONG_X = 4
GROUPS = 1
LOADS = 3
F32 = jnp.float32
BF16 = jnp.bfloat16


def total(value):
    return jnp.sum(jnp.sum(value, axis=1, keepdims=True), axis=0, keepdims=True)


def packed(parts):
    lanes = lax.broadcasted_iota(jnp.int32, (1, 128), 1)
    row = jnp.zeros((1, 128), F32)
    for place, part in enumerate(parts):
        row = jnp.where(lanes == place, part, row)
    return row


def unpacked(row, count):
    lanes = lax.broadcasted_iota(jnp.int32, (1, 128), 1)
    return [
        jnp.sum(jnp.where(lanes == place, row, 0.0), axis=1, keepdims=True) for place in range(count)
    ]


def kernel(
    slabs,
    subs,
    along_x,
    ids_ref,
    count_ref,
    values_hbm,
    side,
    solution_ref,
    residual_ref,
    values,
    columns,
    ids_buf,
    terms,
    sums,
    near,
    far,
    window,
    rows,
    plane,
    depth,
    load_sem,
    ids_send,
    ids_recv,
    term_send,
    term_recv,
    sum_send,
    sum_recv,
    plane_send,
    plane_recv,
    depth_send,
    depth_recv,
):
    tiles = values.shape[0]
    own = 2 * tiles
    nodes = subs * NODES
    slab = lax.axis_index("slab")
    sub = lax.axis_index("sub")
    along_z = slabs // (along_x * CORES)
    core = lax.rem(slab, CORES)
    x_at = lax.rem(slab // CORES, along_x)
    z_at = slab // (CORES * along_x)
    plane_count = along_x * subs
    depth_count = along_z * CORES
    plane_at = x_at * subs + sub
    depth_at = z_at * CORES + core

    def sub_peer(step):
        return (slab, lax.rem(sub + step, subs))

    def slab_peer(step):
        return (lax.rem(slab + step + slabs, slabs), sub)

    def plane_peer(step):
        at = lax.rem(plane_at + step, plane_count)
        return ((z_at * along_x + at // subs) * CORES + core, lax.rem(at, subs))

    def depth_peer(step):
        at = lax.rem(depth_at + step, depth_count)
        return ((at // CORES * along_x + x_at) * CORES + lax.rem(at, CORES), sub)

    def half_of(half):
        return pl.ds(128 * half, 128)

    group = tiles // GROUPS
    share = tiles // LOADS
    loads = []
    for half in range(2):
        for part in range(LOADS):
            at = (pl.ds(part * share, share), slice(None), slice(None), half_of(half))
            loads.append(
                pltpu.make_async_copy(
                    values_hbm.at[at], values.at[at], load_sem.at[half * LOADS + part]
                )
            )
    for load in loads:
        load.start()

    barrier = pltpu.get_barrier_semaphore()
    partners = (
        [slab_peer(step) for step in (-2, -1, 1, 2)]
        + [plane_peer(step) for step in range(1, plane_count)]
        + [depth_peer(step) for step in range(1, depth_count)]
    )
    for partner in partners:
        pl.semaphore_signal(barrier, inc=1, device_id=partner, device_id_type=MESH)

    base = (slab - 1) * nodes
    count = count_ref[0, 0]
    lanes = lax.broadcasted_iota(jnp.int32, (1, 256), 1)
    ids_row = jnp.zeros((1, 256), jnp.int32)
    for tile in range(tiles):
        for slot in range(2):
            mark = ids_ref[slot, tile] - base + 1
            ids_row = jnp.where(lanes == sub * own + 2 * tile + slot, mark, ids_row)
    ids_buf[sub] = ids_row

    live_rows = lax.broadcasted_iota(jnp.int32, (tiles, 128), 0) < count
    residual = jnp.where(live_rows, side[...], 0.0)
    rows[...] = residual
    eye = lax.broadcasted_iota(jnp.int32, (128, 128), 0) == lax.broadcasted_iota(
        jnp.int32, (128, 128), 1
    )
    sent = []

    def copy(source, target, send, recv, peer):
        item = pltpu.make_async_remote_copy(
            src_ref=source,
            dst_ref=target,
            send_sem=send,
            recv_sem=recv,
            device_id=peer,
            device_id_type=MESH,
        )
        item.start()
        sent.append(item)
        return item

    def live_of(tile):
        return jnp.where(tile < count, 1.0, 0.0).astype(F32)

    def place_of(tile, slot):
        return pl.ds(sub * own + 2 * tile + slot, 1)

    def first_tile(tile, half):
        live = live_of(tile)
        if half == 0:
            column = jnp.sum(
                jnp.where(eye, rows[pl.ds(tile, 1), :], 0.0), axis=1, keepdims=True
            )
            column = jnp.broadcast_to(column, (128, 128))
            columns[tile] = column
        else:
            column = columns[tile]
        for slot in range(2):
            block = values[tile, slot, :, 128 * half : 128 * (half + 1)]
            at = place_of(tile, slot)
            terms[0, half, at, :] = jnp.sum(block * column, axis=0, keepdims=True)
            terms[1, half, at, :] = jnp.sum(block * block, axis=0, keepdims=True) * live

    def picked(tile, half):
        live = live_of(tile)
        product = None
        for slot in range(2):
            at = jnp.minimum(jnp.maximum(ids_ref[slot, tile] - base, 0), 3 * nodes - 1)
            row = window[half, pl.ds(at, 1), :] * live
            part = values[tile, slot, :, 128 * half : 128 * (half + 1)] * row
            product = part if product is None else product + part
        return product

    def begin_images():
        @pl.loop(0, tiles, unroll=12)
        def _(tile):
            columns[tile] = picked(tile, 0)

    def image_of(tile):
        column = jnp.sum(columns[tile] + picked(tile, 1), axis=1, keepdims=True)
        rows[pl.ds(tile, 1), :] = jnp.sum(jnp.where(eye, column, 0.0), axis=0, keepdims=True)
        return column

    def back_tile(phase, tile, half):
        if half == 0:
            column = jnp.broadcast_to(image_of(tile), (128, 128))
            columns[tile] = column
        else:
            column = columns[tile]
        for slot in range(2):
            block = values[tile, slot, :, 128 * half : 128 * (half + 1)]
            terms[phase, half, place_of(tile, slot), :] = jnp.sum(
                block * column, axis=0, keepdims=True
            )

    def spread(phase, half, part):
        at = terms.at[phase, half, pl.ds(sub * own + 2 * part * group, 2 * group)]
        return [
            copy(
                at,
                at,
                term_send.at[phase, half, part, step],
                term_recv.at[phase, half, part, step],
                sub_peer(step),
            )
            for step in sorted(range(1, subs), key=lambda step: -min(step, subs - step))
        ]

    def arrived(items):
        for item in items:
            item.wait_recv()

    def summed(value):
        high = value.astype(BF16)
        rest = value - high.astype(F32)
        middle = rest.astype(BF16)
        low = (rest - middle.astype(F32)).astype(BF16)
        return sum(
            jnp.dot(selector, piece, preferred_element_type=F32) for piece in (high, middle, low)
        )

    def exchange(phase, half):
        mine = summed(terms[phase, half])
        sums[phase, half] = mine
        moves = (
            (2, pl.ds(2 * nodes, nodes), far.at[phase, half, 0]),
            (-2, pl.ds(0, nodes), far.at[phase, half, 1]),
            (1, pl.ds(nodes, 2 * nodes), near.at[phase, half, 0]),
            (-1, pl.ds(0, 2 * nodes), near.at[phase, half, 1]),
        )
        items = [
            copy(
                sums.at[phase, half, part],
                target,
                sum_send.at[phase, half, place],
                sum_recv.at[phase, half, place],
                slab_peer(step),
            )
            for place, (step, part, target) in enumerate(moves)
        ]
        return mine, items

    def result(phase, half, moved):
        value, items = moved
        arrived(items)
        below, above = near[phase, half, 0], near[phase, half, 1]
        return jnp.concatenate(
            [
                (far[phase, half, 0] + below[:nodes]) + value[:nodes],
                (below[nodes:] + value[nodes : 2 * nodes]) + above[:nodes],
                (value[2 * nodes :] + above[nodes:]) + far[phase, half, 1],
            ],
            axis=0,
        )

    def start_plane(index, row):
        plane[index, plane_at] = row
        at = plane.at[index, plane_at]
        return [
            copy(at, at, plane_send.at[index, step], plane_recv.at[index, step], plane_peer(step))
            for step in range(1, plane_count)
        ]

    def start_depth(index, items):
        arrived(items)
        depth[index, depth_at] = jnp.sum(plane[index], axis=0)
        at = depth.at[index, depth_at]
        return [
            copy(at, at, depth_send.at[index, step], depth_recv.at[index, step], depth_peer(step))
            for step in range(1, depth_count)
        ]

    def finish_depth(index, items, number):
        arrived(items)
        return unpacked(jnp.sum(depth[index], axis=0), number)

    def middle_of(halves):
        return [half[nodes : 2 * nodes] for half in halves]

    def dot(one, other):
        return total(one[0] * other[0] + one[1] * other[1]) * (1.0 / subs)

    items = {(phase, half): [] for phase in range(2) for half in range(2)}
    for half in range(2):
        for part in range(LOADS):
            loads[half * LOADS + part].wait()

            @pl.loop(part * share, (part + 1) * share, unroll=4)
            def _(tile):
                first_tile(tile, half)

        if half == 0:
            pl.semaphore_wait(barrier, len(partners))
            place = ids_buf.at[sub]
            ids_items = [
                copy(place, place, ids_send.at[step], ids_recv.at[step], sub_peer(step))
                for step in range(1, subs)
            ]
        for phase in range(2):
            items[phase, half] += spread(phase, half, 0)
    arrived(ids_items)
    all_ids = sum(ids_buf[i] for i in range(subs))[:, : subs * own]
    row_ids = lax.broadcasted_iota(jnp.int32, (3 * nodes, subs * own), 0) + 1
    selector = jnp.where(row_ids == all_ids, 1.0, 0.0).astype(BF16)
    moved = {}
    for half in range(2):
        for phase in range(2):
            arrived(items[phase, half])
            moved[phase, half] = exchange(phase, half)
    normal, jacobi, u_all = [], [], []
    for half in range(2):
        normal.append(result(0, half, moved[0, half]))
        jacobi.append(1.0 / (1.0 + result(1, half, moved[1, half])))
        u_all.append(jacobi[half] * normal[half])
        window[half] = u_all[half]
        if half == 0:
            begin_images()

    def applied(phase, meanwhile):
        items = [[], []]
        for half in range(2):
            for part in range(GROUPS):

                @pl.loop(part * group, (part + 1) * group, unroll=12)
                def _(tile):
                    back_tile(phase, tile, half)

                items[half] += spread(phase, half, part)
        found = meanwhile()
        moved = []
        for half in range(2):
            arrived(items[half])
            moved.append(exchange(phase, half))
        return moved, found

    r, u = middle_of(normal), middle_of(u_all)

    def beside_0():
        a_row = rows[...]
        return start_plane(0, packed([dot(r, u), total(a_row * a_row)])), a_row

    moved, (reducing, a_row) = applied(2, beside_0)
    w_all, m_all = [], []
    for half in range(2):
        w_all.append(result(2, half, moved[half]))
        m_all.append(jacobi[half] * w_all[half])
        window[half] = m_all[half]
        if half == 0:
            begin_images()

    w, m = middle_of(w_all), middle_of(m_all)

    def beside_1():
        g_row = rows[...]
        later = start_plane(
            1, packed([dot(w, u), dot(w, m), total(a_row * g_row), total(g_row * g_row)])
        )
        return start_depth(0, reducing), later, g_row

    moved, (reducing, later, g_row) = applied(3, beside_1)
    rho, norm = finish_depth(0, reducing, 2)
    reducing = start_depth(1, later)
    alpha = rho / norm
    z_all = []
    for half in range(2):
        z_all.append(result(3, half, moved[half]))
        w_all[half] = w_all[half] - alpha * z_all[half]
        window[half] = jacobi[half] * w_all[half]
        if half == 0:
            begin_images()
    old_rho, old_norm, old_alpha = rho, norm, alpha

    def beside_2():
        q, s, p = m, w, u
        x = [old_alpha * one for one in p]
        new_u = [one - old_alpha * other for one, other in zip(u, q)]
        new_r = [one - old_alpha * other for one, other in zip(r, s)]
        new_residual = residual - old_alpha * a_row
        new_a = a_row - old_alpha * g_row
        new_w = middle_of(w_all)
        new_m = [jacobi[half][nodes : 2 * nodes] * new_w[half] for half in range(2)]
        return q, s, p, x, new_u, new_r, new_residual, new_a, new_w, new_m, rows[...]

    moved, kept = applied(4, beside_2)
    ap_row, aq_row = a_row, g_row
    q, s, p, x, u, r, residual, a_row, w, m, g_row = kept
    w_u, w_m, a_g, g_g = finish_depth(1, reducing, 4)
    rho = old_rho - 2.0 * old_alpha * w_u + old_alpha * old_alpha * w_m
    beta = rho / old_rho
    lead = 1.0 + beta
    norm = (
        lead * lead * old_norm
        - 2.0 * lead * old_alpha * a_g
        + old_alpha * old_alpha * g_g
    )
    alpha = rho / norm
    q = [one + beta * other for one, other in zip(m, q)]
    s = [one + beta * other for one, other in zip(w, s)]
    p = [one + beta * other for one, other in zip(u, p)]
    x = [one + alpha * other for one, other in zip(x, p)]
    r = [one - alpha * other for one, other in zip(r, s)]
    u = [one - alpha * other for one, other in zip(u, q)]
    ap_row = a_row + beta * ap_row
    aq_row = g_row + beta * aq_row
    residual = residual - alpha * ap_row
    a_row = a_row - alpha * aq_row
    for half in range(2):
        z_all[half] = result(4, half, moved[half]) + beta * z_all[half]
        w_all[half] = w_all[half] - alpha * z_all[half]
        window[half] = jacobi[half] * w_all[half]
        if half == 0:
            begin_images()
    w = middle_of(w_all)
    m = [window[half, pl.ds(nodes, nodes)] for half in range(2)]
    rho_1, norm_1 = rho, norm

    node_dots = [
        dot(r, u),
        dot(w, u),
        dot(w, p),
        dot(s, u),
        dot(w, m),
        dot(s, m),
        dot(s, q),
    ]

    @pl.loop(0, tiles, unroll=24)
    def _(tile):
        image_of(tile)

    g_row = rows[...]
    fields = [a_row, g_row, aq_row, ap_row]
    pairs = [(i, j) for i in range(4) for j in range(i, 4)]
    row_dots = [total(fields[i] * fields[j]) for i, j in pairs]
    before = len(sent)
    planes = start_plane(2, packed(node_dots + row_dots))
    for item in sent[:before]:
        item.wait_send()
    later = start_depth(2, planes)
    for item in planes:
        item.wait_send()
    found = finish_depth(2, later, len(node_dots) + len(pairs))
    rho_2, uu, cross, s_u, w_m, s_m, s_q = found[: len(node_dots)]
    gram = dict(zip(pairs, found[len(node_dots) :]))
    beta = rho_2 / rho_1
    norm_2 = uu + 2.0 * beta * cross + beta * beta * norm_1
    alpha = rho_2 / norm_2
    rho_3 = (
        rho_2
        - 2.0 * alpha * (uu + beta * s_u)
        + alpha * alpha * (w_m + 2.0 * beta * s_m + beta * beta * s_q)
    )
    beta_3 = rho_3 / rho_2
    weights = [1.0 + beta_3, -alpha, -alpha * beta, beta_3 * beta]
    norm_3 = 0.0
    for i, j in pairs:
        norm_3 = norm_3 + (1.0 if i == j else 2.0) * weights[i] * weights[j] * gram[i, j]
    alpha_3 = rho_3 / norm_3
    p = [one + beta * other for one, other in zip(u, p)]
    x = [one + alpha * other for one, other in zip(x, p)]
    u = [one - alpha * (other + beta * last) for one, other, last in zip(u, m, q)]
    p = [one + beta_3 * other for one, other in zip(u, p)]
    x = [one + alpha_3 * other for one, other in zip(x, p)]
    ap_row = a_row + beta * ap_row
    last_row = sum(weights[i] * fields[i] for i in range(4))
    residual_ref[...] = residual - alpha * ap_row - alpha_3 * last_row
    for half in range(2):
        mine = x[half][:NODES]
        for index in range(1, subs):
            mine = jnp.where(sub == index, x[half][index * NODES : (index + 1) * NODES], mine)
        solution_ref[:, 128 * half : 128 * (half + 1)] = mine
    for item in later:
        item.wait_send()


def per_device(slabs, subs, values, block_ids, tile_counts, right_side):
    tiles, coupled, height, width = values.shape
    own = 2 * tiles
    nodes = subs * NODES
    along_x = min(ALONG_X, slabs // CORES)
    plane_count = along_x * subs
    depth_count = slabs // along_x
    half = width // 2
    vmem = pltpu.VMEM
    dma = pltpu.SemaphoreType.DMA
    return pl.pallas_call(
        functools.partial(kernel, slabs, subs, along_x),
        out_shape=(
            jax.ShapeDtypeStruct((NODES, width), F32),
            jax.ShapeDtypeStruct((tiles, height), F32),
        ),
        in_specs=[
            pl.BlockSpec(memory_space=pltpu.SMEM),
            pl.BlockSpec(memory_space=pltpu.SMEM),
            pl.BlockSpec(memory_space=pl.ANY),
            pl.BlockSpec(memory_space=pltpu.VMEM),
        ],
        out_specs=(
            pl.BlockSpec(memory_space=pltpu.VMEM),
            pl.BlockSpec(memory_space=pltpu.VMEM),
        ),
        scratch_shapes=[
            vmem(values.shape, F32),
            vmem((tiles, height, half), F32),
            vmem((subs, 1, 256), jnp.int32),
            vmem((5, 2, subs * own, half), F32),
            vmem((5, 2, 3 * nodes, half), F32),
            vmem((5, 2, 2, 2 * nodes, half), F32),
            vmem((5, 2, 2, nodes, half), F32),
            vmem((2, 3 * nodes, half), F32),
            vmem((tiles, height), F32),
            vmem((3, plane_count, 1, 128), F32),
            vmem((3, depth_count, 1, 128), F32),
            dma((2 * LOADS,)),
            dma((subs,)),
            dma((subs,)),
            dma((5, 2, GROUPS, subs)),
            dma((5, 2, GROUPS, subs)),
            dma((5, 2, 4)),
            dma((5, 2, 4)),
            dma((3, plane_count)),
            dma((3, plane_count)),
            dma((3, depth_count)),
            dma((3, depth_count)),
        ],
        compiler_params=pltpu.CompilerParams(
            collective_id=0, has_side_effects=True, vmem_limit_bytes=48 * 1024 * 1024
        ),
        name="cgls",
    )(block_ids.T, tile_counts, values, right_side)


def solution(mesh):
    both = ("slab", "sub")
    return jax.shard_map(
        functools.partial(per_device, mesh.shape["slab"], mesh.shape["sub"]),
        mesh=mesh,
        in_specs=(P(both, None, None, None), P(both, None), P("slab", "sub"), P(both, None)),
        out_specs=(P(both, None), P(both, None)),
        check_vma=False,
    )
```

```python
import functools

import jax
import jax.numpy as jnp
from jax import lax
from jax.experimental import pallas as pl
from jax.experimental.pallas import tpu as pltpu
from jax.sharding import PartitionSpec as P

MESH = pl.DeviceIdType.MESH
NODES = 12
CORES = 2
ALONG_X = 4
GROUPS = 1
LOADS = 3
F32 = jnp.float32
BF16 = jnp.bfloat16


def total(value):
    return jnp.sum(jnp.sum(value, axis=1, keepdims=True), axis=0, keepdims=True)


def packed(parts):
    lanes = lax.broadcasted_iota(jnp.int32, (1, 128), 1)
    row = jnp.zeros((1, 128), F32)
    for place, part in enumerate(parts):
        row = jnp.where(lanes == place, part, row)
    return row


def unpacked(row, count):
    lanes = lax.broadcasted_iota(jnp.int32, (1, 128), 1)
    return [
        jnp.sum(jnp.where(lanes == place, row, 0.0), axis=1, keepdims=True) for place in range(count)
    ]


def kernel(
    slabs,
    subs,
    along_x,
    ids_ref,
    count_ref,
    values_hbm,
    side,
    solution_ref,
    residual_ref,
    values,
    columns,
    ids_buf,
    terms,
    sums,
    near,
    far,
    window,
    rows,
    plane,
    depth,
    load_sem,
    ids_send,
    ids_recv,
    term_send,
    term_recv,
    sum_send,
    sum_recv,
    plane_send,
    plane_recv,
    depth_send,
    depth_recv,
):
    tiles = values.shape[0]
    own = 2 * tiles
    nodes = subs * NODES
    slab = lax.axis_index("slab")
    sub = lax.axis_index("sub")
    along_z = slabs // (along_x * CORES)
    core = lax.rem(slab, CORES)
    x_at = lax.rem(slab // CORES, along_x)
    z_at = slab // (CORES * along_x)
    plane_count = along_x * subs
    depth_count = along_z * CORES
    plane_at = x_at * subs + sub
    depth_at = z_at * CORES + core

    def sub_peer(step):
        return (slab, lax.rem(sub + step, subs))

    def slab_peer(step):
        return (lax.rem(slab + step + slabs, slabs), sub)

    def plane_peer(step):
        at = lax.rem(plane_at + step, plane_count)
        return ((z_at * along_x + at // subs) * CORES + core, lax.rem(at, subs))

    def depth_peer(step):
        at = lax.rem(depth_at + step, depth_count)
        return ((at // CORES * along_x + x_at) * CORES + lax.rem(at, CORES), sub)

    def half_of(half):
        return pl.ds(128 * half, 128)

    group = tiles // GROUPS
    share = tiles // LOADS
    loads = []
    for half in range(2):
        for part in range(LOADS):
            at = (pl.ds(part * share, share), slice(None), slice(None), half_of(half))
            loads.append(
                pltpu.make_async_copy(
                    values_hbm.at[at], values.at[at], load_sem.at[half * LOADS + part]
                )
            )
    for load in loads:
        load.start()

    barrier = pltpu.get_barrier_semaphore()
    partners = (
        [slab_peer(step) for step in (-2, -1, 1, 2)]
        + [plane_peer(step) for step in range(1, plane_count)]
        + [depth_peer(step) for step in range(1, depth_count)]
    )
    for partner in partners:
        pl.semaphore_signal(barrier, inc=1, device_id=partner, device_id_type=MESH)

    base = (slab - 1) * nodes
    count = count_ref[0, 0]
    lanes = lax.broadcasted_iota(jnp.int32, (1, 256), 1)
    ids_row = jnp.zeros((1, 256), jnp.int32)
    for tile in range(tiles):
        for slot in range(2):
            mark = ids_ref[slot, tile] - base + 1
            ids_row = jnp.where(lanes == sub * own + 2 * tile + slot, mark, ids_row)
    ids_buf[sub] = ids_row

    live_rows = lax.broadcasted_iota(jnp.int32, (tiles, 128), 0) < count
    residual = jnp.where(live_rows, side[...], 0.0)
    rows[...] = residual
    eye = lax.broadcasted_iota(jnp.int32, (128, 128), 0) == lax.broadcasted_iota(
        jnp.int32, (128, 128), 1
    )
    sent = []

    def copy(source, target, send, recv, peer):
        item = pltpu.make_async_remote_copy(
            src_ref=source,
            dst_ref=target,
            send_sem=send,
            recv_sem=recv,
            device_id=peer,
            device_id_type=MESH,
        )
        item.start()
        sent.append(item)
        return item

    def live_of(tile):
        return jnp.where(tile < count, 1.0, 0.0).astype(F32)

    def place_of(tile, slot):
        return pl.ds(sub * own + 2 * tile + slot, 1)

    def first_tile(tile, half):
        live = live_of(tile)
        if half == 0:
            column = jnp.sum(
                jnp.where(eye, rows[pl.ds(tile, 1), :], 0.0), axis=1, keepdims=True
            )
            column = jnp.broadcast_to(column, (128, 128))
            columns[tile] = column
        else:
            column = columns[tile]
        for slot in range(2):
            block = values[tile, slot, :, 128 * half : 128 * (half + 1)]
            at = place_of(tile, slot)
            terms[0, half, at, :] = jnp.sum(block * column, axis=0, keepdims=True)
            terms[1, half, at, :] = jnp.sum(block * block, axis=0, keepdims=True) * live

    def picked(tile, half):
        live = live_of(tile)
        product = None
        for slot in range(2):
            at = jnp.minimum(jnp.maximum(ids_ref[slot, tile] - base, 0), 3 * nodes - 1)
            row = window[half, pl.ds(at, 1), :] * live
            part = values[tile, slot, :, 128 * half : 128 * (half + 1)] * row
            product = part if product is None else product + part
        return product

    def begin_images():
        @pl.loop(0, tiles, unroll=12)
        def _(tile):
            columns[tile] = picked(tile, 0)

    def image_of(tile):
        return jnp.sum(columns[tile] + picked(tile, 1), axis=1, keepdims=True)

    def keep_row(tile, column):
        rows[pl.ds(tile, 1), :] = jnp.sum(jnp.where(eye, column, 0.0), axis=0, keepdims=True)

    def back_tile(phase, tile, half):
        if half == 0:
            column = jnp.broadcast_to(image_of(tile), (128, 128))
            columns[tile] = column
        else:
            column = columns[tile]
        for slot in range(2):
            block = values[tile, slot, :, 128 * half : 128 * (half + 1)]
            terms[phase, half, place_of(tile, slot), :] = jnp.sum(
                block * column, axis=0, keepdims=True
            )

    def spread(phase, half, part):
        at = terms.at[phase, half, pl.ds(sub * own + 2 * part * group, 2 * group)]
        return [
            copy(
                at,
                at,
                term_send.at[phase, half, part, step],
                term_recv.at[phase, half, part, step],
                sub_peer(step),
            )
            for step in sorted(range(1, subs), key=lambda step: -min(step, subs - step))
        ]

    def arrived(items):
        for item in items:
            item.wait_recv()

    def summed(value):
        high = value.astype(BF16)
        rest = value - high.astype(F32)
        middle = rest.astype(BF16)
        low = (rest - middle.astype(F32)).astype(BF16)
        return sum(
            jnp.dot(selector, piece, preferred_element_type=F32) for piece in (high, middle, low)
        )

    def exchange(phase, half):
        mine = summed(terms[phase, half])
        sums[phase, half] = mine
        moves = (
            (2, pl.ds(2 * nodes, nodes), far.at[phase, half, 0]),
            (-2, pl.ds(0, nodes), far.at[phase, half, 1]),
            (1, pl.ds(nodes, 2 * nodes), near.at[phase, half, 0]),
            (-1, pl.ds(0, 2 * nodes), near.at[phase, half, 1]),
        )
        items = [
            copy(
                sums.at[phase, half, part],
                target,
                sum_send.at[phase, half, place],
                sum_recv.at[phase, half, place],
                slab_peer(step),
            )
            for place, (step, part, target) in enumerate(moves)
        ]
        return mine, items

    def result(phase, half, moved):
        value, items = moved
        arrived(items)
        below, above = near[phase, half, 0], near[phase, half, 1]
        return jnp.concatenate(
            [
                (far[phase, half, 0] + below[:nodes]) + value[:nodes],
                (below[nodes:] + value[nodes : 2 * nodes]) + above[:nodes],
                (value[2 * nodes :] + above[nodes:]) + far[phase, half, 1],
            ],
            axis=0,
        )

    def start_plane(index, row):
        plane[index, plane_at] = row
        at = plane.at[index, plane_at]
        return [
            copy(at, at, plane_send.at[index, step], plane_recv.at[index, step], plane_peer(step))
            for step in range(1, plane_count)
        ]

    def start_depth(index, items):
        arrived(items)
        depth[index, depth_at] = jnp.sum(plane[index], axis=0)
        at = depth.at[index, depth_at]
        return [
            copy(at, at, depth_send.at[index, step], depth_recv.at[index, step], depth_peer(step))
            for step in range(1, depth_count)
        ]

    def finish_depth(index, items, number):
        arrived(items)
        return unpacked(jnp.sum(depth[index], axis=0), number)

    def middle_of(halves):
        return [half[nodes : 2 * nodes] for half in halves]

    def dot(one, other):
        return total(one[0] * other[0] + one[1] * other[1]) * (1.0 / subs)

    items = {(phase, half): [] for phase in range(2) for half in range(2)}
    for half in range(2):
        for part in range(LOADS):
            loads[half * LOADS + part].wait()

            @pl.loop(part * share, (part + 1) * share, unroll=4)
            def _(tile):
                first_tile(tile, half)

        if half == 0:
            pl.semaphore_wait(barrier, len(partners))
            place = ids_buf.at[sub]
            ids_items = [
                copy(place, place, ids_send.at[step], ids_recv.at[step], sub_peer(step))
                for step in range(1, subs)
            ]
        for phase in range(2):
            items[phase, half] += spread(phase, half, 0)
    arrived(ids_items)
    all_ids = sum(ids_buf[i] for i in range(subs))[:, : subs * own]
    row_ids = lax.broadcasted_iota(jnp.int32, (3 * nodes, subs * own), 0) + 1
    selector = jnp.where(row_ids == all_ids, 1.0, 0.0).astype(BF16)
    moved = {}
    for half in range(2):
        for phase in range(2):
            arrived(items[phase, half])
            moved[phase, half] = exchange(phase, half)
    normal, jacobi, u_all = [], [], []
    for half in range(2):
        normal.append(result(0, half, moved[0, half]))
        jacobi.append(1.0 / (1.0 + result(1, half, moved[1, half])))
        u_all.append(jacobi[half] * normal[half])
        window[half] = u_all[half]
        if half == 0:
            begin_images()

    def applied(phase, meanwhile):
        items = [[], []]
        for half in range(2):
            for part in range(GROUPS):

                @pl.loop(part * group, (part + 1) * group, unroll=12)
                def _(tile):
                    back_tile(phase, tile, half)

                items[half] += spread(phase, half, part)

        @pl.loop(0, tiles, unroll=12)
        def _(tile):
            keep_row(tile, columns[tile])

        found = meanwhile()
        moved = []
        for half in range(2):
            arrived(items[half])
            moved.append(exchange(phase, half))
        return moved, found

    r, u = middle_of(normal), middle_of(u_all)

    def beside_0():
        a_row = rows[...]
        return start_plane(0, packed([dot(r, u), total(a_row * a_row)])), a_row

    moved, (reducing, a_row) = applied(2, beside_0)
    w_all, m_all = [], []
    for half in range(2):
        w_all.append(result(2, half, moved[half]))
        m_all.append(jacobi[half] * w_all[half])
        window[half] = m_all[half]
        if half == 0:
            begin_images()

    w, m = middle_of(w_all), middle_of(m_all)

    def beside_1():
        g_row = rows[...]
        later = start_plane(
            1, packed([dot(w, u), dot(w, m), total(a_row * g_row), total(g_row * g_row)])
        )
        return start_depth(0, reducing), later, g_row

    moved, (reducing, later, g_row) = applied(3, beside_1)
    rho, norm = finish_depth(0, reducing, 2)
    reducing = start_depth(1, later)
    alpha = rho / norm
    z_all = []
    for half in range(2):
        z_all.append(result(3, half, moved[half]))
        w_all[half] = w_all[half] - alpha * z_all[half]
        window[half] = jacobi[half] * w_all[half]
        if half == 0:
            begin_images()
    old_rho, old_norm, old_alpha = rho, norm, alpha

    def beside_2():
        q, s, p = m, w, u
        x = [old_alpha * one for one in p]
        new_u = [one - old_alpha * other for one, other in zip(u, q)]
        new_r = [one - old_alpha * other for one, other in zip(r, s)]
        new_residual = residual - old_alpha * a_row
        new_a = a_row - old_alpha * g_row
        new_w = middle_of(w_all)
        new_m = [jacobi[half][nodes : 2 * nodes] * new_w[half] for half in range(2)]
        return q, s, p, x, new_u, new_r, new_residual, new_a, new_w, new_m, rows[...]

    moved, kept = applied(4, beside_2)
    ap_row, aq_row = a_row, g_row
    q, s, p, x, u, r, residual, a_row, w, m, g_row = kept
    w_u, w_m, a_g, g_g = finish_depth(1, reducing, 4)
    rho = old_rho - 2.0 * old_alpha * w_u + old_alpha * old_alpha * w_m
    beta = rho / old_rho
    lead = 1.0 + beta
    norm = (
        lead * lead * old_norm
        - 2.0 * lead * old_alpha * a_g
        + old_alpha * old_alpha * g_g
    )
    alpha = rho / norm
    q = [one + beta * other for one, other in zip(m, q)]
    s = [one + beta * other for one, other in zip(w, s)]
    p = [one + beta * other for one, other in zip(u, p)]
    x = [one + alpha * other for one, other in zip(x, p)]
    r = [one - alpha * other for one, other in zip(r, s)]
    u = [one - alpha * other for one, other in zip(u, q)]
    ap_row = a_row + beta * ap_row
    aq_row = g_row + beta * aq_row
    residual = residual - alpha * ap_row
    a_row = a_row - alpha * aq_row
    for half in range(2):
        z_all[half] = result(4, half, moved[half]) + beta * z_all[half]
        w_all[half] = w_all[half] - alpha * z_all[half]
        window[half] = jacobi[half] * w_all[half]
        if half == 0:
            begin_images()
    w = middle_of(w_all)
    m = [window[half, pl.ds(nodes, nodes)] for half in range(2)]
    rho_1, norm_1 = rho, norm

    node_dots = [
        dot(r, u),
        dot(w, u),
        dot(w, p),
        dot(s, u),
        dot(w, m),
        dot(s, m),
        dot(s, q),
    ]

    @pl.loop(0, tiles, unroll=24)
    def _(tile):
        keep_row(tile, image_of(tile))

    g_row = rows[...]
    fields = [a_row, g_row, aq_row, ap_row]
    pairs = [(i, j) for i in range(4) for j in range(i, 4)]
    row_dots = [total(fields[i] * fields[j]) for i, j in pairs]
    before = len(sent)
    planes = start_plane(2, packed(node_dots + row_dots))
    for item in sent[:before]:
        item.wait_send()
    later = start_depth(2, planes)
    for item in planes:
        item.wait_send()
    found = finish_depth(2, later, len(node_dots) + len(pairs))
    rho_2, uu, cross, s_u, w_m, s_m, s_q = found[: len(node_dots)]
    gram = dict(zip(pairs, found[len(node_dots) :]))
    beta = rho_2 / rho_1
    norm_2 = uu + 2.0 * beta * cross + beta * beta * norm_1
    alpha = rho_2 / norm_2
    rho_3 = (
        rho_2
        - 2.0 * alpha * (uu + beta * s_u)
        + alpha * alpha * (w_m + 2.0 * beta * s_m + beta * beta * s_q)
    )
    beta_3 = rho_3 / rho_2
    weights = [1.0 + beta_3, -alpha, -alpha * beta, beta_3 * beta]
    norm_3 = 0.0
    for i, j in pairs:
        norm_3 = norm_3 + (1.0 if i == j else 2.0) * weights[i] * weights[j] * gram[i, j]
    alpha_3 = rho_3 / norm_3
    p = [one + beta * other for one, other in zip(u, p)]
    x = [one + alpha * other for one, other in zip(x, p)]
    u = [one - alpha * (other + beta * last) for one, other, last in zip(u, m, q)]
    p = [one + beta_3 * other for one, other in zip(u, p)]
    x = [one + alpha_3 * other for one, other in zip(x, p)]
    ap_row = a_row + beta * ap_row
    last_row = sum(weights[i] * fields[i] for i in range(4))
    residual_ref[...] = residual - alpha * ap_row - alpha_3 * last_row
    for half in range(2):
        mine = x[half][:NODES]
        for index in range(1, subs):
            mine = jnp.where(sub == index, x[half][index * NODES : (index + 1) * NODES], mine)
        solution_ref[:, 128 * half : 128 * (half + 1)] = mine
    for item in later:
        item.wait_send()


def per_device(slabs, subs, values, block_ids, tile_counts, right_side):
    tiles, coupled, height, width = values.shape
    own = 2 * tiles
    nodes = subs * NODES
    along_x = min(ALONG_X, slabs // CORES)
    plane_count = along_x * subs
    depth_count = slabs // along_x
    half = width // 2
    vmem = pltpu.VMEM
    dma = pltpu.SemaphoreType.DMA
    return pl.pallas_call(
        functools.partial(kernel, slabs, subs, along_x),
        out_shape=(
            jax.ShapeDtypeStruct((NODES, width), F32),
            jax.ShapeDtypeStruct((tiles, height), F32),
        ),
        in_specs=[
            pl.BlockSpec(memory_space=pltpu.SMEM),
            pl.BlockSpec(memory_space=pltpu.SMEM),
            pl.BlockSpec(memory_space=pl.ANY),
            pl.BlockSpec(memory_space=pltpu.VMEM),
        ],
        out_specs=(
            pl.BlockSpec(memory_space=pltpu.VMEM),
            pl.BlockSpec(memory_space=pltpu.VMEM),
        ),
        scratch_shapes=[
            vmem(values.shape, F32),
            vmem((tiles, height, half), F32),
            vmem((subs, 1, 256), jnp.int32),
            vmem((5, 2, subs * own, half), F32),
            vmem((5, 2, 3 * nodes, half), F32),
            vmem((5, 2, 2, 2 * nodes, half), F32),
            vmem((5, 2, 2, nodes, half), F32),
            vmem((2, 3 * nodes, half), F32),
            vmem((tiles, height), F32),
            vmem((3, plane_count, 1, 128), F32),
            vmem((3, depth_count, 1, 128), F32),
            dma((2 * LOADS,)),
            dma((subs,)),
            dma((subs,)),
            dma((5, 2, GROUPS, subs)),
            dma((5, 2, GROUPS, subs)),
            dma((5, 2, 4)),
            dma((5, 2, 4)),
            dma((3, plane_count)),
            dma((3, plane_count)),
            dma((3, depth_count)),
            dma((3, depth_count)),
        ],
        compiler_params=pltpu.CompilerParams(
            collective_id=0, has_side_effects=True, vmem_limit_bytes=48 * 1024 * 1024
        ),
        name="cgls",
    )(block_ids.T, tile_counts, values, right_side)


def solution(mesh):
    both = ("slab", "sub")
    return jax.shard_map(
        functools.partial(per_device, mesh.shape["slab"], mesh.shape["sub"]),
        mesh=mesh,
        in_specs=(P(both, None, None, None), P(both, None), P("slab", "sub"), P(both, None)),
        out_specs=(P(both, None), P(both, None)),
        check_vma=False,
    )
```

```python
import functools

import jax
import jax.numpy as jnp
from jax import lax
from jax.experimental import pallas as pl
from jax.experimental.pallas import tpu as pltpu
from jax.sharding import PartitionSpec as P

MESH = pl.DeviceIdType.MESH
NODES = 12
CORES = 2
ALONG_X = 4
GROUPS = 1
LOADS = 3
F32 = jnp.float32
BF16 = jnp.bfloat16


def total(value):
    return jnp.sum(jnp.sum(value, axis=1, keepdims=True), axis=0, keepdims=True)


def packed(parts):
    lanes = lax.broadcasted_iota(jnp.int32, (1, 128), 1)
    row = jnp.zeros((1, 128), F32)
    for place, part in enumerate(parts):
        row = jnp.where(lanes == place, part, row)
    return row


def unpacked(row, count):
    lanes = lax.broadcasted_iota(jnp.int32, (1, 128), 1)
    return [
        jnp.sum(jnp.where(lanes == place, row, 0.0), axis=1, keepdims=True) for place in range(count)
    ]


def kernel(
    slabs,
    subs,
    along_x,
    ids_ref,
    count_ref,
    values_hbm,
    side,
    solution_ref,
    residual_ref,
    values,
    columns,
    ids_buf,
    terms,
    sums,
    near,
    far,
    window,
    rows,
    plane,
    depth,
    load_sem,
    ids_send,
    ids_recv,
    term_send,
    term_recv,
    sum_send,
    sum_recv,
    plane_send,
    plane_recv,
    depth_send,
    depth_recv,
):
    tiles = values.shape[0]
    own = 2 * tiles
    nodes = subs * NODES
    slab = lax.axis_index("slab")
    sub = lax.axis_index("sub")
    along_z = slabs // (along_x * CORES)
    core = lax.rem(slab, CORES)
    x_at = lax.rem(slab // CORES, along_x)
    z_at = slab // (CORES * along_x)
    plane_count = along_x * subs
    depth_count = along_z * CORES
    plane_at = x_at * subs + sub
    depth_at = z_at * CORES + core

    def sub_peer(step):
        return (slab, lax.rem(sub + step, subs))

    def slab_peer(step):
        return (lax.rem(slab + step + slabs, slabs), sub)

    def plane_peer(step):
        at = lax.rem(plane_at + step, plane_count)
        return ((z_at * along_x + at // subs) * CORES + core, lax.rem(at, subs))

    def depth_peer(step):
        at = lax.rem(depth_at + step, depth_count)
        return ((at // CORES * along_x + x_at) * CORES + lax.rem(at, CORES), sub)

    def half_of(half):
        return pl.ds(128 * half, 128)

    group = tiles // GROUPS
    share = tiles // LOADS
    loads = []
    for half in range(2):
        for part in range(LOADS):
            at = (pl.ds(part * share, share), slice(None), slice(None), half_of(half))
            loads.append(
                pltpu.make_async_copy(
                    values_hbm.at[at], values.at[at], load_sem.at[half * LOADS + part]
                )
            )
    for load in loads:
        load.start()

    barrier = pltpu.get_barrier_semaphore()
    partners = (
        [slab_peer(step) for step in (-2, -1, 1, 2)]
        + [plane_peer(step) for step in range(1, plane_count)]
        + [depth_peer(step) for step in range(1, depth_count)]
    )
    for partner in partners:
        pl.semaphore_signal(barrier, inc=1, device_id=partner, device_id_type=MESH)

    base = (slab - 1) * nodes
    count = count_ref[0, 0]
    lanes = lax.broadcasted_iota(jnp.int32, (1, 256), 1)
    ids_row = jnp.zeros((1, 256), jnp.int32)
    for tile in range(tiles):
        for slot in range(2):
            mark = ids_ref[slot, tile] - base + 1
            ids_row = jnp.where(lanes == sub * own + 2 * tile + slot, mark, ids_row)
    ids_buf[sub] = ids_row

    live_rows = lax.broadcasted_iota(jnp.int32, (tiles, 128), 0) < count
    residual = jnp.where(live_rows, side[...], 0.0)
    rows[...] = residual
    eye = lax.broadcasted_iota(jnp.int32, (128, 128), 0) == lax.broadcasted_iota(
        jnp.int32, (128, 128), 1
    )
    sent = []

    def copy(source, target, send, recv, peer):
        item = pltpu.make_async_remote_copy(
            src_ref=source,
            dst_ref=target,
            send_sem=send,
            recv_sem=recv,
            device_id=peer,
            device_id_type=MESH,
        )
        item.start()
        sent.append(item)
        return item

    def live_of(tile):
        return jnp.where(tile < count, 1.0, 0.0).astype(F32)

    def place_of(tile, slot):
        return pl.ds(sub * own + 2 * tile + slot, 1)

    def first_tile(tile, half):
        live = live_of(tile)
        if half == 0:
            column = jnp.sum(
                jnp.where(eye, rows[pl.ds(tile, 1), :], 0.0), axis=1, keepdims=True
            )
            column = jnp.broadcast_to(column, (128, 128))
            columns[tile] = column
        else:
            column = columns[tile]
        for slot in range(2):
            block = values[tile, slot, :, 128 * half : 128 * (half + 1)]
            at = place_of(tile, slot)
            terms[0, half, at, :] = jnp.sum(block * column, axis=0, keepdims=True)
            terms[1, half, at, :] = jnp.sum(block * block, axis=0, keepdims=True) * live

    def picked(tile, half):
        live = live_of(tile)
        product = None
        for slot in range(2):
            at = jnp.minimum(jnp.maximum(ids_ref[slot, tile] - base, 0), 3 * nodes - 1)
            row = window[half, pl.ds(at, 1), :] * live
            part = values[tile, slot, :, 128 * half : 128 * (half + 1)] * row
            product = part if product is None else product + part
        return product

    def begin_images():
        @pl.loop(0, tiles, unroll=12)
        def _(tile):
            columns[tile] = picked(tile, 0)

    def image_of(tile):
        return jnp.sum(columns[tile] + picked(tile, 1), axis=1, keepdims=True)

    def keep_row(tile, column):
        rows[pl.ds(tile, 1), :] = jnp.sum(jnp.where(eye, column, 0.0), axis=0, keepdims=True)

    def back_tile(phase, tile, half):
        if half == 0:
            column = jnp.broadcast_to(image_of(tile), (128, 128))
            columns[tile] = column
        else:
            column = columns[tile]
        for slot in range(2):
            block = values[tile, slot, :, 128 * half : 128 * (half + 1)]
            terms[phase, half, place_of(tile, slot), :] = jnp.sum(
                block * column, axis=0, keepdims=True
            )

    def spread(phase, half, part):
        at = terms.at[phase, half, pl.ds(sub * own + 2 * part * group, 2 * group)]
        return [
            copy(
                at,
                at,
                term_send.at[phase, half, part, step],
                term_recv.at[phase, half, part, step],
                sub_peer(step),
            )
            for step in sorted(range(1, subs), key=lambda step: -min(step, subs - step))
        ]

    def arrived(items):
        for item in items:
            item.wait_recv()

    def summed(value):
        high = value.astype(BF16)
        rest = value - high.astype(F32)
        middle = rest.astype(BF16)
        low = (rest - middle.astype(F32)).astype(BF16)
        return sum(
            jnp.dot(selector, piece, preferred_element_type=F32) for piece in (high, middle, low)
        )

    def exchange(phase, half):
        mine = summed(terms[phase, half])
        sums[phase, half] = mine
        moves = (
            (2, pl.ds(2 * nodes, nodes), far.at[phase, half, 0]),
            (-2, pl.ds(0, nodes), far.at[phase, half, 1]),
            (1, pl.ds(nodes, 2 * nodes), near.at[phase, half, 0]),
            (-1, pl.ds(0, 2 * nodes), near.at[phase, half, 1]),
        )
        items = [
            copy(
                sums.at[phase, half, part],
                target,
                sum_send.at[phase, half, place],
                sum_recv.at[phase, half, place],
                slab_peer(step),
            )
            for place, (step, part, target) in enumerate(moves)
        ]
        return mine, items

    def result(phase, half, moved):
        value, items = moved
        arrived(items)
        below, above = near[phase, half, 0], near[phase, half, 1]
        return jnp.concatenate(
            [
                (far[phase, half, 0] + below[:nodes]) + value[:nodes],
                (below[nodes:] + value[nodes : 2 * nodes]) + above[:nodes],
                (value[2 * nodes :] + above[nodes:]) + far[phase, half, 1],
            ],
            axis=0,
        )

    def start_plane(index, row):
        plane[index, plane_at] = row
        at = plane.at[index, plane_at]
        return [
            copy(at, at, plane_send.at[index, step], plane_recv.at[index, step], plane_peer(step))
            for step in range(1, plane_count)
        ]

    def start_depth(index, items):
        arrived(items)
        depth[index, depth_at] = jnp.sum(plane[index], axis=0)
        at = depth.at[index, depth_at]
        return [
            copy(at, at, depth_send.at[index, step], depth_recv.at[index, step], depth_peer(step))
            for step in range(1, depth_count)
        ]

    def finish_depth(index, items, number):
        arrived(items)
        return unpacked(jnp.sum(depth[index], axis=0), number)

    def middle_of(halves):
        return [half[nodes : 2 * nodes] for half in halves]

    def dot(one, other):
        return total(one[0] * other[0] + one[1] * other[1]) * (1.0 / subs)

    items = {(phase, half): [] for phase in range(2) for half in range(2)}
    for half in range(2):
        for part in range(LOADS):
            loads[half * LOADS + part].wait()

            @pl.loop(part * share, (part + 1) * share, unroll=8)
            def _(tile):
                first_tile(tile, half)

        if half == 0:
            pl.semaphore_wait(barrier, len(partners))
            place = ids_buf.at[sub]
            ids_items = [
                copy(place, place, ids_send.at[step], ids_recv.at[step], sub_peer(step))
                for step in range(1, subs)
            ]
        for phase in range(2):
            items[phase, half] += spread(phase, half, 0)
    arrived(ids_items)
    all_ids = sum(ids_buf[i] for i in range(subs))[:, : subs * own]
    row_ids = lax.broadcasted_iota(jnp.int32, (3 * nodes, subs * own), 0) + 1
    selector = jnp.where(row_ids == all_ids, 1.0, 0.0).astype(BF16)
    moved = {}
    for half in range(2):
        for phase in range(2):
            arrived(items[phase, half])
            moved[phase, half] = exchange(phase, half)
    normal, jacobi, u_all = [], [], []
    for half in range(2):
        normal.append(result(0, half, moved[0, half]))
        jacobi.append(1.0 / (1.0 + result(1, half, moved[1, half])))
        u_all.append(jacobi[half] * normal[half])
        window[half] = u_all[half]
        if half == 0:
            begin_images()

    def applied(phase, meanwhile):
        items = [[], []]
        for half in range(2):
            for part in range(GROUPS):

                @pl.loop(part * group, (part + 1) * group, unroll=24)
                def _(tile):
                    back_tile(phase, tile, half)

                items[half] += spread(phase, half, part)

        @pl.loop(0, tiles, unroll=12)
        def _(tile):
            keep_row(tile, columns[tile])

        found = meanwhile()
        moved = []
        for half in range(2):
            arrived(items[half])
            moved.append(exchange(phase, half))
        return moved, found

    r, u = middle_of(normal), middle_of(u_all)

    def beside_0():
        a_row = rows[...]
        return start_plane(0, packed([dot(r, u), total(a_row * a_row)])), a_row

    moved, (reducing, a_row) = applied(2, beside_0)
    w_all, m_all = [], []
    for half in range(2):
        w_all.append(result(2, half, moved[half]))
        m_all.append(jacobi[half] * w_all[half])
        window[half] = m_all[half]
        if half == 0:
            begin_images()

    w, m = middle_of(w_all), middle_of(m_all)

    def beside_1():
        g_row = rows[...]
        later = start_plane(
            1, packed([dot(w, u), dot(w, m), total(a_row * g_row), total(g_row * g_row)])
        )
        return start_depth(0, reducing), later, g_row

    moved, (reducing, later, g_row) = applied(3, beside_1)
    rho, norm = finish_depth(0, reducing, 2)
    reducing = start_depth(1, later)
    alpha = rho / norm
    z_all = []
    for half in range(2):
        z_all.append(result(3, half, moved[half]))
        w_all[half] = w_all[half] - alpha * z_all[half]
        window[half] = jacobi[half] * w_all[half]
        if half == 0:
            begin_images()
    old_rho, old_norm, old_alpha = rho, norm, alpha

    def beside_2():
        q, s, p = m, w, u
        x = [old_alpha * one for one in p]
        new_u = [one - old_alpha * other for one, other in zip(u, q)]
        new_r = [one - old_alpha * other for one, other in zip(r, s)]
        new_residual = residual - old_alpha * a_row
        new_a = a_row - old_alpha * g_row
        new_w = middle_of(w_all)
        new_m = [jacobi[half][nodes : 2 * nodes] * new_w[half] for half in range(2)]
        return q, s, p, x, new_u, new_r, new_residual, new_a, new_w, new_m, rows[...]

    moved, kept = applied(4, beside_2)
    ap_row, aq_row = a_row, g_row
    q, s, p, x, u, r, residual, a_row, w, m, g_row = kept
    w_u, w_m, a_g, g_g = finish_depth(1, reducing, 4)
    rho = old_rho - 2.0 * old_alpha * w_u + old_alpha * old_alpha * w_m
    beta = rho / old_rho
    lead = 1.0 + beta
    norm = (
        lead * lead * old_norm
        - 2.0 * lead * old_alpha * a_g
        + old_alpha * old_alpha * g_g
    )
    alpha = rho / norm
    q = [one + beta * other for one, other in zip(m, q)]
    s = [one + beta * other for one, other in zip(w, s)]
    p = [one + beta * other for one, other in zip(u, p)]
    x = [one + alpha * other for one, other in zip(x, p)]
    r = [one - alpha * other for one, other in zip(r, s)]
    u = [one - alpha * other for one, other in zip(u, q)]
    ap_row = a_row + beta * ap_row
    aq_row = g_row + beta * aq_row
    residual = residual - alpha * ap_row
    a_row = a_row - alpha * aq_row
    for half in range(2):
        z_all[half] = result(4, half, moved[half]) + beta * z_all[half]
        w_all[half] = w_all[half] - alpha * z_all[half]
        window[half] = jacobi[half] * w_all[half]
        if half == 0:
            begin_images()
    w = middle_of(w_all)
    m = [window[half, pl.ds(nodes, nodes)] for half in range(2)]
    rho_1, norm_1 = rho, norm

    node_dots = [
        dot(r, u),
        dot(w, u),
        dot(w, p),
        dot(s, u),
        dot(w, m),
        dot(s, m),
        dot(s, q),
    ]

    @pl.loop(0, tiles, unroll=24)
    def _(tile):
        keep_row(tile, image_of(tile))

    g_row = rows[...]
    fields = [a_row, g_row, aq_row, ap_row]
    pairs = [(i, j) for i in range(4) for j in range(i, 4)]
    row_dots = [total(fields[i] * fields[j]) for i, j in pairs]
    before = len(sent)
    planes = start_plane(2, packed(node_dots + row_dots))
    for item in sent[:before]:
        item.wait_send()
    later = start_depth(2, planes)
    for item in planes:
        item.wait_send()
    found = finish_depth(2, later, len(node_dots) + len(pairs))
    rho_2, uu, cross, s_u, w_m, s_m, s_q = found[: len(node_dots)]
    gram = dict(zip(pairs, found[len(node_dots) :]))
    beta = rho_2 / rho_1
    norm_2 = uu + 2.0 * beta * cross + beta * beta * norm_1
    alpha = rho_2 / norm_2
    rho_3 = (
        rho_2
        - 2.0 * alpha * (uu + beta * s_u)
        + alpha * alpha * (w_m + 2.0 * beta * s_m + beta * beta * s_q)
    )
    beta_3 = rho_3 / rho_2
    weights = [1.0 + beta_3, -alpha, -alpha * beta, beta_3 * beta]
    norm_3 = 0.0
    for i, j in pairs:
        norm_3 = norm_3 + (1.0 if i == j else 2.0) * weights[i] * weights[j] * gram[i, j]
    alpha_3 = rho_3 / norm_3
    p = [one + beta * other for one, other in zip(u, p)]
    x = [one + alpha * other for one, other in zip(x, p)]
    u = [one - alpha * (other + beta * last) for one, other, last in zip(u, m, q)]
    p = [one + beta_3 * other for one, other in zip(u, p)]
    x = [one + alpha_3 * other for one, other in zip(x, p)]
    ap_row = a_row + beta * ap_row
    last_row = sum(weights[i] * fields[i] for i in range(4))
    residual_ref[...] = residual - alpha * ap_row - alpha_3 * last_row
    for half in range(2):
        mine = x[half][:NODES]
        for index in range(1, subs):
            mine = jnp.where(sub == index, x[half][index * NODES : (index + 1) * NODES], mine)
        solution_ref[:, 128 * half : 128 * (half + 1)] = mine
    for item in later:
        item.wait_send()


def per_device(slabs, subs, values, block_ids, tile_counts, right_side):
    tiles, coupled, height, width = values.shape
    own = 2 * tiles
    nodes = subs * NODES
    along_x = min(ALONG_X, slabs // CORES)
    plane_count = along_x * subs
    depth_count = slabs // along_x
    half = width // 2
    vmem = pltpu.VMEM
    dma = pltpu.SemaphoreType.DMA
    return pl.pallas_call(
        functools.partial(kernel, slabs, subs, along_x),
        out_shape=(
            jax.ShapeDtypeStruct((NODES, width), F32),
            jax.ShapeDtypeStruct((tiles, height), F32),
        ),
        in_specs=[
            pl.BlockSpec(memory_space=pltpu.SMEM),
            pl.BlockSpec(memory_space=pltpu.SMEM),
            pl.BlockSpec(memory_space=pl.ANY),
            pl.BlockSpec(memory_space=pltpu.VMEM),
        ],
        out_specs=(
            pl.BlockSpec(memory_space=pltpu.VMEM),
            pl.BlockSpec(memory_space=pltpu.VMEM),
        ),
        scratch_shapes=[
            vmem(values.shape, F32),
            vmem((tiles, height, half), F32),
            vmem((subs, 1, 256), jnp.int32),
            vmem((5, 2, subs * own, half), F32),
            vmem((5, 2, 3 * nodes, half), F32),
            vmem((5, 2, 2, 2 * nodes, half), F32),
            vmem((5, 2, 2, nodes, half), F32),
            vmem((2, 3 * nodes, half), F32),
            vmem((tiles, height), F32),
            vmem((3, plane_count, 1, 128), F32),
            vmem((3, depth_count, 1, 128), F32),
            dma((2 * LOADS,)),
            dma((subs,)),
            dma((subs,)),
            dma((5, 2, GROUPS, subs)),
            dma((5, 2, GROUPS, subs)),
            dma((5, 2, 4)),
            dma((5, 2, 4)),
            dma((3, plane_count)),
            dma((3, plane_count)),
            dma((3, depth_count)),
            dma((3, depth_count)),
        ],
        compiler_params=pltpu.CompilerParams(
            collective_id=0, has_side_effects=True, vmem_limit_bytes=48 * 1024 * 1024
        ),
        name="cgls",
    )(block_ids.T, tile_counts, values, right_side)


def solution(mesh):
    both = ("slab", "sub")
    return jax.shard_map(
        functools.partial(per_device, mesh.shape["slab"], mesh.shape["sub"]),
        mesh=mesh,
        in_specs=(P(both, None, None, None), P(both, None), P("slab", "sub"), P(both, None)),
        out_specs=(P(both, None), P(both, None)),
        check_vma=False,
    )
```
